32 devices in a mesh: groups: 2 (over y), det: 4 (over z), tm: 4 (over x, core).
Axes of the slice: x: 2, y: 2, z: 4, core: 2. Of those that a mesh axis runs over, the one named last changes fastest.
Arguments:
- tod: float32 [2048, 16384], P(('groups', 'det'), 'tm'), parts along dimension 0, may hold values from -8 to 8
- gain_knots: float32 [2048, 64], P(('groups', 'det')), parts along dimension 0, may hold values from 0.25 to 1.75
- intervals: int32 [32768], P(('groups', 'tm')), parts along dimension 0, may hold values from 0 to 62, never falling along the last dimension, each value on 1 to 1040 neighbouring positions
- fraction: float32 [32768], P(('groups', 'tm')), parts along dimension 0, may hold values from 0 to 1
- azimuth: int32 [32768], P(('groups', 'tm')), parts along dimension 0, may hold values from 0 to 447
- mode_index: int32 [32], P(('groups', 'tm')), parts along dimension 0, may hold values from 0 to 1
- mode_bank: float32 [2, 1024, 512], P(None, 'det'), may hold values from -0.1875 to 0.1875
- mode_mix: float32 [2, 512, 512], replicated, may hold values from -0.2 to 0.2
Outputs:
- filtered: float32 [2048, 16384], P(('groups', 'det'), 'tm'), parts along dimension 0
The draws below stay inside these ranges and needn't reach their ends.
There are 2 independent parts, one for each index of `groups`. The reference program is written for one: setup_inputs(seed, part) draws one part's arguments, and reference() takes and returns one part's arrays. A program takes and returns all parts, laid end to end along the dimension named above; an argument that names none is the same for every part. Nothing has to cross between parts.
Inputs may be any that keep to these rules, and one draw needn't show every extreme that they name: `intervals`: never falls along time; every interval from 0 to 62 holds at least one sample.
All inputs are finite; a program needn't handle non-finite values.
Results may differ from the reference program's by a relative error of at most 0.000068.
Values sent between devices are 32-bit elements; how exact they have to be, the bound alone decides.
No kernel may reach another device: no remote copies, remote signals or barrier semaphores. Data moves between devices by JAX's collectives and lax.ppermute only.
A program may use at most 128 MiB of HBM per device.

```python
import math
import jax
import jax.numpy as jnp
import numpy as np
from jax import lax

BLOCK = 1024
M = 512
NBIN = 512
NKNOT = 64
NBANK = 2
NDET = 1024
NS = 16384
NBLK = 16


def with_ends(array, key, smallest, largest):
    longest = array.shape.index(max(array.shape))
    spots = []
    for shift in (0, 1):
        where = [jax.random.randint(jax.random.fold_in(key, axis), (), 0, length) for axis, length in enumerate(array.shape)]
        where[longest] = (where[longest] + shift) % array.shape[longest]
        spots.append(tuple(where))
    return array.at[spots[0]].set(smallest).at[spots[1]].set(largest)


def level_of(key, extent, pieces, low, top_value):
    def one(axis_at, blocks):
        heights = jax.random.uniform(jax.random.fold_in(jax.random.fold_in(key, 6), axis_at), (blocks,), jnp.float32, low / len(pieces), top_value / len(pieces))
        return jnp.repeat(jnp.exp(heights), extent[axis_at] // blocks).reshape((-1,) + (1,) * (len(extent) - axis_at - 1))

    level = one(*pieces[0])
    for cut in pieces[1:]:
        level = level * one(*cut)
    return level


def profile(number_of, total, bound, slope):
    portions = [(1 << 20) // math.isqrt(grade ** slope) + 1 for grade in range(2, number_of + 1)]
    surplus, given = total - bound - (number_of - 1), [1] * (number_of - 1)
    while surplus > 0:
        free = [i for i in range(number_of - 1) if given[i] < bound]
        pool, left = sum([portions[i] for i in free]), surplus
        for i in free:
            addition = min(bound - given[i], max(1, left * portions[i] // pool), surplus)
            given[i] = given[i] + addition
            surplus = surplus - addition
    return np.array([bound] + given)


def ragged(stream_key, amount, total, reach, slope):
    if amount == 2:
        one = jax.random.randint(stream_key, (), max(1, total - reach), min(reach, total - 1) + 1)
        return jnp.stack([one, total - one])
    lengths = jnp.asarray(profile(amount, total, reach, slope), jnp.int32)
    pairs = (amount - 1) // 2
    donor, taker = lengths[1:1 + 2 * pairs:2], lengths[2:2 + 2 * pairs:2]
    room = jnp.minimum(donor - 1, reach - taker)
    shifted = jax.random.randint(jax.random.fold_in(stream_key, 1), (pairs,), 0, 1 << 20) % (room + 1)
    lengths = lengths.at[1:1 + 2 * pairs:2].set(donor - shifted).at[2:2 + 2 * pairs:2].set(taker + shifted)
    return lengths[jax.random.permutation(jax.random.fold_in(stream_key, 2), amount)]


def centred(key, dims, width, reach, pieces=(), kind=jnp.bfloat16):
    factor_of = level_of(key, dims, pieces, -0.22, 0.18) if pieces else 1.0
    drawn = jax.random.normal(key, dims, jnp.float32) * width * factor_of
    return jnp.minimum(jnp.maximum(drawn, -reach), reach).astype(kind)


def setup_inputs(seed: int = 0, part: int = 0) -> dict:
    splits = jax.random.split(jax.random.key(seed), 9)
    own_keys = jax.random.split(jax.random.fold_in(splits[8], part), 9)
    return {
        "tod": centred(own_keys[0], (NDET, NS), 1.0, 8.0, ((0, 4), (1, 4)), jnp.float32),
        "gain_knots": jnp.clip(1.0 + 0.15 * jax.random.normal(own_keys[1], (NDET, NKNOT), jnp.float32), 0.25, 1.75),
        "intervals": jnp.searchsorted(jnp.cumsum(ragged(own_keys[2], NKNOT - 1, NS, 4 * NS // (NKNOT - 1), 0)), jnp.arange(NS), side="right").astype(jnp.int32),
        "fraction": jnp.clip(1.0 * jax.random.uniform(own_keys[3], (NS,), jnp.float32) ** level_of(own_keys[3], (NS,), ((0, 4),), -0.2, 0.2), 0.0, 1.0),
        "azimuth": with_ends(jax.random.randint(own_keys[4], (NS,), 0, NBIN - NBIN // 8), jax.random.fold_in(own_keys[4], 1), 0, (NBIN - NBIN // 8) - 1).astype(jnp.int32),
        "mode_index": with_ends(jax.random.randint(own_keys[5], (NBLK,), 0, NBANK), jax.random.fold_in(own_keys[5], 1), 0, NBANK - 1).astype(jnp.int32),
        "mode_bank": centred(splits[6], (NBANK, NDET, M), NDET ** -0.5, 0.1875, ((1, 4),), jnp.float32),
        "mode_mix": centred(splits[7], (NBANK, M, M), 0.03, 0.2, (), jnp.float32),
    }


def reference(tod, gain_knots, intervals, fraction, azimuth, mode_index, mode_bank, mode_mix):
    precise = lax.Precision.HIGHEST
    knot_row = lax.broadcasted_iota(jnp.int32, (NKNOT, NS), 0)
    spread = jnp.where(knot_row == intervals[None, :], 1.0 - fraction[None, :], 0.0)
    spread = spread + jnp.where(knot_row == intervals[None, :] + 1, fraction[None, :], 0.0)
    calibrated = tod * jnp.dot(gain_knots, spread, precision=precise)
    blocks = calibrated.reshape(NDET, NBLK, BLOCK).transpose(1, 0, 2)

    def clean_block(item):
        data, which = item
        modes = mode_bank[which]
        amps = jnp.dot(modes.T, data, precision=precise)
        coef = amps + jnp.dot(mode_mix[which], amps, precision=precise)
        return data - jnp.dot(modes, coef, precision=precise)

    cleaned = lax.map(clean_block, (blocks, mode_index)).transpose(1, 0, 2).reshape(NDET, NS)
    onehot = (lax.broadcasted_iota(jnp.int32, (NBIN, NS), 0) == azimuth[None, :]).astype(tod.dtype)
    fit = lax.dot_general(cleaned, onehot, (((1,), (1,)), ((), ())), precision=precise)
    counts = jnp.sum(onehot, axis=1)
    template = fit / jnp.maximum(counts, 1.0)[None, :]
    return cleaned - jnp.dot(template, onehot, precision=precise)
```

```python
import functools
import jax
import jax.numpy as jnp
from jax import lax
from jax.experimental import pallas as pl
from jax.experimental.pallas import tpu as pltpu
from jax.sharding import PartitionSpec as P

BLOCK = 1024
NBIN = 512
PIECES = ((0, 256), (512, 512), (256, 256))


def gathered_sums(tod, gain_knots, intervals, fraction, azimuth, mode_index, mode_bank, mode_mix):
    precise = lax.Precision.HIGHEST
    det_rows, samples = tod.shape
    knot_row = lax.broadcasted_iota(jnp.int32, (gain_knots.shape[1], samples), 0)
    spread = jnp.where(knot_row == intervals[None, :], 1.0 - fraction[None, :], 0.0)
    spread = spread + jnp.where(knot_row == intervals[None, :] + 1, fraction[None, :], 0.0)
    calibrated = tod * jnp.dot(gain_knots, spread, precision=precise)
    nblocks = samples // BLOCK
    blocks = calibrated.reshape(det_rows, nblocks, BLOCK)
    selected = jnp.take(mode_bank, mode_index, axis=0)
    mixing = jnp.take(mode_mix, mode_index, axis=0)
    partial_amps = jnp.einsum("kdm,dkt->kmt", selected, blocks, precision=precise)
    share = lax.psum_scatter(partial_amps, "det", scatter_dimension=2, tiled=True)
    coef_share = share + jnp.einsum("kmn,knt->kmt", mixing, share, precision=precise)
    coef = lax.all_gather(coef_share, "det", axis=2, tiled=True)
    removed = jnp.einsum("kdm,kmt->dkt", selected, coef, precision=precise)
    cleaned = (blocks - removed).reshape(det_rows, samples)
    onehot = (lax.broadcasted_iota(jnp.int32, (NBIN, samples), 0) == azimuth[None, :]).astype(
        tod.dtype
    )
    fit_part = lax.dot_general(cleaned, onehot, (((1,), (1,)), ((), ())), precision=precise)
    count_part = jnp.sum(onehot, axis=1)
    fit, counts = lax.psum((fit_part, count_part), "tm")
    template = fit / jnp.maximum(counts, 1.0)[None, :]
    return cleaned - jnp.dot(template, onehot, precision=precise)


def halves(x):
    high = x.astype(jnp.bfloat16)
    return high, (x - high.astype(jnp.float32)).astype(jnp.bfloat16)


def dot(a, b, contract=((1,), (0,))):
    return lax.dot_general(a, b, (contract, ((), ())), preferred_element_type=jnp.float32)


def dot3(a, b):
    return dot(a[0], b[0]) + (dot(a[0], b[1]) + dot(a[1], b[0]))


def calibrate_kernel(count, me_ref, gain_ref, *refs):
    gain_high, gain_low = halves(gain_ref[...])
    gains = jnp.concatenate([gain_high, gain_high, gain_low, gain_low], axis=0)
    knots = gain_ref.shape[0]
    for n in range(count):
        tod_ref, where_ref, share_ref = refs[3 * n : 3 * n + 3]
        knot_row = lax.broadcasted_iota(jnp.int32, (knots, tod_ref.shape[1]), 0)
        where, share = where_ref[...], share_ref[...]
        spread = jnp.where(knot_row == where, 1.0 - share, 0.0)
        spread = spread + jnp.where(knot_row == where + 1, share, 0.0)
        high, low = halves(spread)
        spreads = jnp.concatenate([high, low, high, low], axis=0)
        refs[3 * count + n][...] = tod_ref[...] * dot(gains, spreads, ((0,), (0,)))


def calibrate(ring, me, tod, gains, where, share, pieces):
    rows = tod.shape[0]
    specs, operands = [], []
    for shift, start, width in pieces:
        per_block, offset = BLOCK // width, start // width

        def at(i, me_ref, shift=shift, per_block=per_block, offset=offset):
            return 0, lax.rem(me_ref[0] + shift, ring) * per_block + offset

        specs += [pl.BlockSpec((rows, width), at)] + [pl.BlockSpec((1, width), at)] * 2
        operands += [tod, where, share]
    return pl.pallas_call(
        functools.partial(calibrate_kernel, len(pieces)),
        out_shape=[jax.ShapeDtypeStruct((rows, width), jnp.float32) for _, _, width in pieces],
        grid_spec=pltpu.PrefetchScalarGridSpec(
            num_scalar_prefetch=1,
            grid=(1,),
            in_specs=[pl.BlockSpec(gains.shape, lambda i, me_ref: (0, 0))] + specs,
            out_specs=[pl.BlockSpec((rows, width), lambda i, me_ref: (0, 0)) for _, _, width in pieces],
        ),
        cost_estimate=pl.CostEstimate(
            flops=2 * rows * 256 * sum(w for _, _, w in pieces),
            bytes_accessed=8 * rows * sum(w for _, _, w in pieces),
            transcendentals=0,
        ),
    )(me, gains, *operands)


def modes_kernel(ring, shares, at_ref, bank_ref, mix_ref, first_high, first_low, second_high, second_low, modes):
    rows = bank_ref.shape[2]
    me, part = at_ref[0], at_ref[2]
    other = jnp.bitwise_xor(me, lax.rem(me - pl.program_id(0) + ring, ring))
    z_slot = (other // 2) + 2 * lax.rem(other, 2)
    for share in range(shares):
        flip = jnp.bitwise_xor(part, share)
        slot = z_slot + ring * (lax.rem(flip // 2, 2) + 2 * (flip // 4) + 4 * lax.rem(flip, 2))
        modes[pl.ds(share * rows, rows), :] = bank_ref[slot, 0]
    u = modes[...]
    mixed = u + dot3(halves(u), halves(mix_ref[0]))
    first_high[...], first_low[...] = halves(u.T)
    second_high[...], second_low[...] = halves(mixed)


def prepare_modes(ring, shares, at, banks, mode_mix):
    _, _, rows, m = banks.shape
    det_rows = rows * shares
    first = pl.BlockSpec((m, det_rows), lambda s, at_ref: (0, s))
    second = pl.BlockSpec((det_rows, m), lambda s, at_ref: (s, 0))
    total = ring * det_rows
    return pl.pallas_call(
        functools.partial(modes_kernel, ring, shares),
        out_shape=[jax.ShapeDtypeStruct((m, total), jnp.bfloat16)] * 2
        + [jax.ShapeDtypeStruct((total, m), jnp.bfloat16)] * 2,
        grid_spec=pltpu.PrefetchScalarGridSpec(
            num_scalar_prefetch=1,
            grid=(ring,),
            in_specs=[
                pl.BlockSpec((banks.shape[0], 1, rows, m), lambda s, at_ref: (0, at_ref[1], 0, 0)),
                pl.BlockSpec((1, m, m), lambda s, at_ref: (at_ref[1], 0, 0)),
            ],
            out_specs=[first, first, second, second],
            scratch_shapes=[pltpu.VMEM((det_rows, m), jnp.float32)],
        ),
        cost_estimate=pl.CostEstimate(
            flops=6 * total * m * m, bytes_accessed=12 * total * m, transcendentals=0
        ),
    )(at, banks, mode_mix)


def filter_kernel(ring, first_high, first_low, second_high, second_low, *refs):
    rows = refs[0].shape[0]
    data = halves(jnp.concatenate([refs[s][...] for s in range(ring)], axis=0))
    amps = dot3((first_high[...], first_low[...]), data)
    amps = halves(amps)
    for s in range(ring):
        block = pl.ds(s * rows, rows)
        refs[ring + s][...] = dot3((second_high[block, :], second_low[block, :]), amps)


def common_mode(ring, modes, arrived):
    rows, width = arrived[0].shape
    m, total = modes[0].shape
    tile = min(width, 256)
    whole = [pl.BlockSpec((m, total), lambda i: (0, 0))] * 2 + [pl.BlockSpec((total, m), lambda i: (0, 0))] * 2
    column = pl.BlockSpec((rows, tile), lambda i: (0, i))
    return pl.pallas_call(
        functools.partial(filter_kernel, ring),
        out_shape=[jax.ShapeDtypeStruct((rows, width), jnp.float32)] * ring,
        grid=(width // tile,),
        in_specs=whole + [column] * ring,
        out_specs=[column] * ring,
        cost_estimate=pl.CostEstimate(
            flops=12 * total * m * width, bytes_accessed=8 * total * width, transcendentals=0
        ),
    )(*modes, *arrived)


def fit_kernel(ring, more, at_ref, *refs):
    data, back, azimuth_ref = refs[:ring], refs[ring : 2 * ring], refs[2 * ring]
    old = refs[2 * ring + 1 : 2 * ring + 3] if more else ()
    cleaned_ref, fit_ref = refs[-2:]
    step = pl.program_id(0)

    @pl.when(step == 0)
    def _():
        fit_ref[...] = old[1][...] if more else jnp.zeros_like(fit_ref)

    for s in range(ring):

        @pl.when(step == s)
        def _():
            cleaned_ref[...] = data[s][...] - back[s][...]

    rows = cleaned_ref.shape[0]
    cleaned = jnp.concatenate(halves(cleaned_ref[...]), axis=0)
    bins = lax.broadcasted_iota(jnp.int32, (fit_ref.shape[1], cleaned_ref.shape[1]), 0)
    onehot = (bins == azimuth_ref[...]).astype(jnp.float32).astype(jnp.bfloat16)
    sums = dot(cleaned, onehot, ((1,), (1,)))
    fit_ref[...] += sums[:rows] + sums[rows:]


def fit_piece(ring, at, start, data, back, azimuth, old):
    rows, width = data[0].shape
    samples = azimuth.shape[1]
    per_block, offset = BLOCK // width, start // width

    def where(s, at_ref):
        return 0, lax.rem(at_ref[0] + s, ring) * per_block + offset

    full = pl.BlockSpec((rows, width), lambda s, at_ref: (0, 0))
    sums = pl.BlockSpec((rows, NBIN), lambda s, at_ref: (0, 0))
    more = old is not None
    return pl.pallas_call(
        functools.partial(fit_kernel, ring, more),
        out_shape=[
            jax.ShapeDtypeStruct((rows, samples), jnp.float32),
            jax.ShapeDtypeStruct((rows, NBIN), jnp.float32),
        ],
        grid_spec=pltpu.PrefetchScalarGridSpec(
            num_scalar_prefetch=1,
            grid=(ring,),
            in_specs=[full] * (2 * ring)
            + [pl.BlockSpec((1, width), where)]
            + ([pl.BlockSpec(memory_space=pl.ANY), sums] if more else []),
            out_specs=[pl.BlockSpec((rows, width), where), sums],
        ),
        input_output_aliases={2 * ring + 2: 0} if more else {},
        cost_estimate=pl.CostEstimate(
            flops=4 * ring * rows * width * NBIN, bytes_accessed=12 * ring * rows * width, transcendentals=0
        ),
    )(at, *data, *back, azimuth, *(old if more else ()))


def template_kernel(at_ref, cleaned_ref, azimuth_ref, own_ref, mate_ref, counts_ref, out_ref, both_ref):
    half = own_ref.shape[0]
    core = at_ref[3]

    @pl.when(pl.program_id(0) == 0)
    def _():
        counts = jnp.maximum(counts_ref[...], 1.0)
        for ref, side in ((own_ref, core), (mate_ref, 1 - core)):
            first = pl.multiple_of(side * half, half)
            high, low = halves(ref[...] / counts)
            both_ref[pl.ds(first, half), :] = high
            both_ref[pl.ds(2 * half + first, half), :] = low

    bins = lax.broadcasted_iota(jnp.int32, (both_ref.shape[1], cleaned_ref.shape[1]), 0)
    onehot = (bins == azimuth_ref[...]).astype(jnp.float32).astype(jnp.bfloat16)
    template = dot(both_ref[...], onehot)
    out_ref[...] = cleaned_ref[...] - (template[: 2 * half] + template[2 * half :])


def remove_template(at, cleaned, azimuth, own, mate, counts):
    rows, samples = cleaned.shape
    tile = 512
    column = pl.BlockSpec((rows, tile), lambda i, at_ref: (0, i))
    whole = pl.BlockSpec(own.shape, lambda i, at_ref: (0, 0))
    return pl.pallas_call(
        template_kernel,
        out_shape=jax.ShapeDtypeStruct((rows, samples), jnp.float32),
        grid_spec=pltpu.PrefetchScalarGridSpec(
            num_scalar_prefetch=1,
            grid=(samples // tile,),
            in_specs=[
                column,
                pl.BlockSpec((1, tile), lambda i, at_ref: (0, i)),
                whole,
                whole,
                pl.BlockSpec(counts.shape, lambda i, at_ref: (0, 0)),
            ],
            out_specs=column,
            scratch_shapes=[pltpu.VMEM((2 * rows, own.shape[1]), jnp.bfloat16)],
        ),
        cost_estimate=pl.CostEstimate(
            flops=4 * rows * samples * NBIN, bytes_accessed=8 * rows * samples, transcendentals=0
        ),
    )(at, cleaned, azimuth, own, mate, counts)


def exchanged_blocks(ring, shares, tod, gain_knots, intervals, fraction, azimuth, mode_index, mode_bank, mode_mix):
    det_rows, samples = tod.shape
    me = lax.axis_index("det")
    tm = lax.axis_index("tm")
    part_of = lax.axis_index("groups") * lax.axis_size("tm") + tm
    core = lax.rem(tm, 2)
    which = lax.dynamic_index_in_dim(mode_index, me, 0, False)
    me_only = jnp.full((1,), me, jnp.int32)
    at = jnp.stack([me, which, part_of, core])

    def send(array, shift):
        return lax.ppermute(array, "det", [(i, (i + shift) % ring) for i in range(ring)])

    def swap(array, axis, bit):
        return lax.ppermute(array, axis, [(i, i ^ bit) for i in range(lax.axis_size(axis))])

    gains = gain_knots.T
    where, share = intervals[None, :], fraction[None, :]
    azimuth = azimuth[None, :]
    data, arrived = {}, {}
    order = [[(s, start, width) for s in (1, 2, 3)] for start, width in PIECES]
    order[-1] += [(0, start, width) for start, width in PIECES]
    for pieces in order:
        blocks = calibrate(ring, me_only, tod, gains, where, share, pieces)
        for (s, start, width), block in zip(pieces, blocks):
            data[s, start] = block
            arrived[s, start] = send(block, s) if s else block

    rows = det_rows // shares
    banks = lax.dynamic_slice_in_dim(mode_bank, part_of * rows, rows, 1)[None]
    for axis, bit in (("det", 2), ("det", 1), ("tm", 2), ("groups", 1), ("tm", 1)):
        banks = jnp.concatenate([banks, swap(banks, axis, bit)], axis=0)
    modes = prepare_modes(ring, shares, at, banks, mode_mix)

    counts = jnp.sum((lax.broadcasted_iota(jnp.int32, (NBIN, samples), 0) == azimuth).astype(jnp.float32), axis=1)
    counts = jnp.broadcast_to(counts[None, :], (8, NBIN))
    for bit in (1, 2):
        counts = counts + swap(counts, "tm", bit)

    state = None
    for start, width in PIECES:
        removed = common_mode(ring, modes, [arrived[s, start] for s in range(ring)])
        back = [send(removed[s], -s) if s else removed[s] for s in range(ring)]
        state = fit_piece(ring, at, start, [data[s, start] for s in range(ring)], back, azimuth, state)
    cleaned, fit = state
    half = det_rows // 2
    own = lax.dynamic_slice_in_dim(fit, core * half, half, 0)
    own = own + swap(lax.dynamic_slice_in_dim(fit, (1 - core) * half, half, 0), "tm", 1)
    own = own + swap(own, "tm", 2)
    mate = swap(own, "tm", 1)
    return remove_template(at, cleaned, azimuth, own, mate, counts[:1])


def solution(mesh):
    placed = (
        P(("groups", "det"), "tm"),
        P(("groups", "det"), None),
        P(("groups", "tm")),
        P(("groups", "tm")),
        P(("groups", "tm")),
        P(("groups", "tm")),
        P(None, "det", None),
        P(),
    )
    ring = mesh.shape["det"]
    shares = mesh.shape["groups"] * mesh.shape["tm"]

    def on_device(tod, gain_knots, intervals, fraction, azimuth, mode_index, mode_bank, mode_mix):
        args = (tod, gain_knots, intervals, fraction, azimuth, mode_index, mode_bank, mode_mix)
        if ring == 4 and mode_index.shape[0] == ring and shares == 8 and tod.shape[0] % (16 * shares) == 0:
            return exchanged_blocks(ring, shares, *args)
        return gathered_sums(*args)

    return jax.shard_map(
        on_device, mesh=mesh, in_specs=placed, out_specs=P(("groups", "det"), "tm"), check_vma=False
    )
```

```python
import functools
import jax
import jax.numpy as jnp
from jax import lax
from jax.experimental import pallas as pl
from jax.experimental.pallas import tpu as pltpu
from jax.sharding import PartitionSpec as P

BLOCK = 1024
NBIN = 512
PIECES = ((0, 256), (512, 512), (256, 256))


def gathered_sums(tod, gain_knots, intervals, fraction, azimuth, mode_index, mode_bank, mode_mix):
    precise = lax.Precision.HIGHEST
    det_rows, samples = tod.shape
    knot_row = lax.broadcasted_iota(jnp.int32, (gain_knots.shape[1], samples), 0)
    spread = jnp.where(knot_row == intervals[None, :], 1.0 - fraction[None, :], 0.0)
    spread = spread + jnp.where(knot_row == intervals[None, :] + 1, fraction[None, :], 0.0)
    calibrated = tod * jnp.dot(gain_knots, spread, precision=precise)
    nblocks = samples // BLOCK
    blocks = calibrated.reshape(det_rows, nblocks, BLOCK)
    selected = jnp.take(mode_bank, mode_index, axis=0)
    mixing = jnp.take(mode_mix, mode_index, axis=0)
    partial_amps = jnp.einsum("kdm,dkt->kmt", selected, blocks, precision=precise)
    share = lax.psum_scatter(partial_amps, "det", scatter_dimension=2, tiled=True)
    coef_share = share + jnp.einsum("kmn,knt->kmt", mixing, share, precision=precise)
    coef = lax.all_gather(coef_share, "det", axis=2, tiled=True)
    removed = jnp.einsum("kdm,kmt->dkt", selected, coef, precision=precise)
    cleaned = (blocks - removed).reshape(det_rows, samples)
    onehot = (lax.broadcasted_iota(jnp.int32, (NBIN, samples), 0) == azimuth[None, :]).astype(
        tod.dtype
    )
    fit_part = lax.dot_general(cleaned, onehot, (((1,), (1,)), ((), ())), precision=precise)
    count_part = jnp.sum(onehot, axis=1)
    fit, counts = lax.psum((fit_part, count_part), "tm")
    template = fit / jnp.maximum(counts, 1.0)[None, :]
    return cleaned - jnp.dot(template, onehot, precision=precise)


def halves(x):
    high = x.astype(jnp.bfloat16)
    return high, (x - high.astype(jnp.float32)).astype(jnp.bfloat16)


def dot(a, b, contract=((1,), (0,))):
    return lax.dot_general(a, b, (contract, ((), ())), preferred_element_type=jnp.float32)


def dot3(a, b):
    return dot(a[0], b[0]) + (dot(a[0], b[1]) + dot(a[1], b[0]))


def calibrate_kernel(count, me_ref, gain_ref, *refs):
    gain_high, gain_low = halves(gain_ref[...])
    gains = jnp.concatenate([gain_high, gain_high, gain_low, gain_low], axis=0)
    knots = gain_ref.shape[0]
    for n in range(count):
        tod_ref, where_ref, share_ref = refs[3 * n : 3 * n + 3]
        knot_row = lax.broadcasted_iota(jnp.int32, (knots, tod_ref.shape[1]), 0)
        where, share = where_ref[...], share_ref[...]
        spread = jnp.where(knot_row == where, 1.0 - share, 0.0)
        spread = spread + jnp.where(knot_row == where + 1, share, 0.0)
        high, low = halves(spread)
        spreads = jnp.concatenate([high, low, high, low], axis=0)
        refs[3 * count + n][...] = tod_ref[...] * dot(gains, spreads, ((0,), (0,)))


def calibrate(ring, me, tod, gains, where, share, pieces):
    rows = tod.shape[0]
    specs, operands = [], []
    for shift, start, width in pieces:
        per_block, offset = BLOCK // width, start // width

        def at(i, me_ref, shift=shift, per_block=per_block, offset=offset):
            return 0, lax.rem(me_ref[0] + shift, ring) * per_block + offset

        specs += [pl.BlockSpec((rows, width), at)] + [pl.BlockSpec((1, width), at)] * 2
        operands += [tod, where, share]
    return pl.pallas_call(
        functools.partial(calibrate_kernel, len(pieces)),
        out_shape=[jax.ShapeDtypeStruct((rows, width), jnp.float32) for _, _, width in pieces],
        grid_spec=pltpu.PrefetchScalarGridSpec(
            num_scalar_prefetch=1,
            grid=(1,),
            in_specs=[pl.BlockSpec(gains.shape, lambda i, me_ref: (0, 0))] + specs,
            out_specs=[pl.BlockSpec((rows, width), lambda i, me_ref: (0, 0)) for _, _, width in pieces],
        ),
        cost_estimate=pl.CostEstimate(
            flops=2 * rows * 256 * sum(w for _, _, w in pieces),
            bytes_accessed=8 * rows * sum(w for _, _, w in pieces),
            transcendentals=0,
        ),
    )(me, gains, *operands)


def modes_kernel(ring, shares, at_ref, bank_ref, mix_ref, first_high, first_low, second_high, second_low, modes):
    rows = bank_ref.shape[2]
    me, part = at_ref[0], at_ref[2]
    other = jnp.bitwise_xor(me, lax.rem(me - pl.program_id(0) + ring, ring))
    z_slot = (other // 2) + 2 * lax.rem(other, 2)
    for share in range(shares):
        flip = jnp.bitwise_xor(part, share)
        slot = z_slot + ring * (lax.rem(flip // 2, 2) + 2 * (flip // 4) + 4 * lax.rem(flip, 2))
        modes[pl.ds(share * rows, rows), :] = bank_ref[slot, 0]
    u = modes[...]
    mixed = u + dot3(halves(u), halves(mix_ref[0]))
    first_high[...], first_low[...] = halves(u.T)
    second_high[...], second_low[...] = halves(mixed)


def prepare_modes(ring, shares, at, banks, mode_mix):
    _, _, rows, m = banks.shape
    det_rows = rows * shares
    first = pl.BlockSpec((m, det_rows), lambda s, at_ref: (0, s))
    second = pl.BlockSpec((det_rows, m), lambda s, at_ref: (s, 0))
    total = ring * det_rows
    return pl.pallas_call(
        functools.partial(modes_kernel, ring, shares),
        out_shape=[jax.ShapeDtypeStruct((m, total), jnp.bfloat16)] * 2
        + [jax.ShapeDtypeStruct((total, m), jnp.bfloat16)] * 2,
        grid_spec=pltpu.PrefetchScalarGridSpec(
            num_scalar_prefetch=1,
            grid=(ring,),
            in_specs=[
                pl.BlockSpec((banks.shape[0], 1, rows, m), lambda s, at_ref: (0, at_ref[1], 0, 0)),
                pl.BlockSpec((1, m, m), lambda s, at_ref: (at_ref[1], 0, 0)),
            ],
            out_specs=[first, first, second, second],
            scratch_shapes=[pltpu.VMEM((det_rows, m), jnp.float32)],
        ),
        cost_estimate=pl.CostEstimate(
            flops=6 * total * m * m, bytes_accessed=12 * total * m, transcendentals=0
        ),
    )(at, banks, mode_mix)


def filter_kernel(ring, first_high, first_low, second_high, second_low, *refs):
    rows = refs[0].shape[0]
    data = halves(jnp.concatenate([refs[s][...] for s in range(ring)], axis=0))
    amps = dot3((first_high[...], first_low[...]), data)
    amps = halves(amps)
    for s in range(ring):
        block = pl.ds(s * rows, rows)
        refs[ring + s][...] = dot3((second_high[block, :], second_low[block, :]), amps)


def common_mode(ring, modes, arrived):
    rows, width = arrived[0].shape
    m, total = modes[0].shape
    tile = min(width, 256)
    whole = [pl.BlockSpec((m, total), lambda i: (0, 0))] * 2 + [pl.BlockSpec((total, m), lambda i: (0, 0))] * 2
    column = pl.BlockSpec((rows, tile), lambda i: (0, i))
    return pl.pallas_call(
        functools.partial(filter_kernel, ring),
        out_shape=[jax.ShapeDtypeStruct((rows, width), jnp.float32)] * ring,
        grid=(width // tile,),
        in_specs=whole + [column] * ring,
        out_specs=[column] * ring,
        cost_estimate=pl.CostEstimate(
            flops=12 * total * m * width, bytes_accessed=8 * total * width, transcendentals=0
        ),
    )(*modes, *arrived)


def onehot_of(azimuth, bins):
    row = lax.broadcasted_iota(jnp.int32, (bins, azimuth.shape[1]), 0)
    return (row == azimuth).astype(jnp.float32).astype(jnp.bfloat16)


def block_start(ring, me, shift, start):
    return pl.multiple_of(lax.rem(me + shift, ring) * BLOCK + start, 128)


def bin_kernel(ring, pieces, at_ref, index_ref, azimuth_ref, *refs):
    data, (keep_ref, send_ref, sums) = refs[: len(pieces)], refs[len(pieces) :]
    me, tm = at_ref[0], at_ref[4]
    rows = keep_ref.shape[0]
    sums[...] = jnp.zeros_like(sums)
    for (shift, start, width), ref in zip(pieces, data):
        both = jnp.concatenate(halves(ref[...]), axis=0)
        onehot = onehot_of(azimuth_ref[:, pl.ds(block_start(ring, me, shift, start), width)], sums.shape[2])
        part = dot(both, onehot, ((1,), (1,)))
        sums[index_ref[lax.rem(me + shift, ring)]] += part[:rows] + part[rows:]
    share = sums.shape[2] // 4
    for x in range(2):
        for bank in range(2):
            column = slice((2 * x + bank) * share, (2 * x + bank + 1) * share)
            for flip, ref in ((0, keep_ref), (1, send_ref)):
                first = pl.multiple_of(jnp.bitwise_xor(tm, 2 * x + flip) * share, share)
                ref[:, column] = sums[bank, :, pl.ds(first, share)]


def bin_data(ring, at, mode_index, azimuth, pieces, data):
    rows = data[0].shape[0]
    work = sum(width for _, _, width in pieces)
    return pl.pallas_call(
        functools.partial(bin_kernel, ring, pieces),
        out_shape=[jax.ShapeDtypeStruct((rows, NBIN), jnp.float32)] * 2,
        in_specs=[pl.BlockSpec(memory_space=pltpu.SMEM)] * 2 + [pl.BlockSpec(memory_space=pltpu.VMEM)] * (1 + len(data)),
        out_specs=[pl.BlockSpec(memory_space=pltpu.VMEM)] * 2,
        scratch_shapes=[pltpu.VMEM((2, rows, NBIN), jnp.float32)],
        cost_estimate=pl.CostEstimate(
            flops=4 * rows * work * NBIN, bytes_accessed=4 * rows * work, transcendentals=0
        ),
    )(at, mode_index, azimuth, *data)


def pool_kernel(ring, shares, at_ref, bank_ref, own_ref, mix_ref, sums_ref, mine_ref, cross_ref, near_ref, total):
    step = pl.program_id(0)
    slots, _, rows, m = bank_ref.shape
    sums = halves(sums_ref[...])
    amps = [halves(own_ref[0].T)[n] for n in range(2)]
    amps = dot3(amps, sums)
    coef = halves(amps + dot3(halves(mix_ref[0]), halves(amps)))
    removed = dot3(halves(bank_ref[:, 0].reshape(slots * rows, m)), coef)

    @pl.when(step == 0)
    def _():
        total[...] = removed
        mine_ref[...] = sums_ref[...]

    @pl.when(step == 1)
    def _():
        total[...] += removed
        mine_ref[...] += sums_ref[...]
        part = at_ref[2]
        for p in range(shares):
            flip = jnp.bitwise_xor(part, p)
            slot = ring * (lax.rem(flip // 2, 2) + 2 * (flip // 4) + 4 * lax.rem(flip, 2))
            block = slice(p * rows, (p + 1) * rows)

            def rows_of(z):
                return total[pl.ds(pl.multiple_of((slot + z) * rows, rows), rows), :]

            mine_ref[block, :] -= rows_of(0)
            cross_ref[block, :] = rows_of(1)
            near_ref[block, :] = rows_of(2)
            near_ref[p * rows + shares * rows : (p + 1) * rows + shares * rows, :] = rows_of(3)


def pool(ring, shares, at, banks, mode_bank, mode_mix, sums):
    slots, _, rows, m = banks.shape
    det_rows, share = rows * shares, sums.shape[1] // 2
    shapes = [(det_rows, share), (det_rows, share), (2 * det_rows, share)]
    return pl.pallas_call(
        functools.partial(pool_kernel, ring, shares),
        out_shape=[jax.ShapeDtypeStruct(shape, jnp.float32) for shape in shapes],
        grid_spec=pltpu.PrefetchScalarGridSpec(
            num_scalar_prefetch=1,
            grid=(2,),
            in_specs=[
                pl.BlockSpec((slots, 1, rows, m), lambda b, at_ref: (0, b, 0, 0)),
                pl.BlockSpec((1, det_rows, m), lambda b, at_ref: (b, 0, 0)),
                pl.BlockSpec((1, m, m), lambda b, at_ref: (b, 0, 0)),
                pl.BlockSpec((det_rows, share), lambda b, at_ref: (0, b)),
            ],
            out_specs=[pl.BlockSpec(shape, lambda b, at_ref: (0, 0)) for shape in shapes],
            scratch_shapes=[pltpu.VMEM((slots * rows, share), jnp.float32)],
        ),
        cost_estimate=pl.CostEstimate(
            flops=30 * slots * rows * m * share, bytes_accessed=8 * slots * rows * m, transcendentals=0
        ),
    )(at, banks, mode_bank, mode_mix, sums)


def stack_kernel(at_ref, here_ref, there_ref, counts_ref, both_ref):
    tm = at_ref[4]
    rows, width = here_ref.shape
    share = width // 2
    for flip, ref in ((0, here_ref), (1, there_ref)):
        for x in range(2):
            first = pl.multiple_of(jnp.bitwise_xor(tm, 2 * x + flip) * share, share)
            counts = jnp.maximum(counts_ref[:1, pl.ds(first, share)], 1.0)
            high, low = halves(ref[:, x * share : (x + 1) * share] / counts)
            both_ref[:rows, pl.ds(first, share)] = high
            both_ref[rows:, pl.ds(first, share)] = low


def stack_template(at, here, there, counts):
    return pl.pallas_call(
        stack_kernel,
        out_shape=jax.ShapeDtypeStruct((2 * here.shape[0], NBIN), jnp.bfloat16),
        in_specs=[pl.BlockSpec(memory_space=pltpu.SMEM)] + [pl.BlockSpec(memory_space=pltpu.VMEM)] * 3,
        out_specs=pl.BlockSpec(memory_space=pltpu.VMEM),
    )(at, here, there, counts)


def finish_kernel(ring, count, template, at_ref, *refs):
    data, back, refs, out_ref = refs[:ring], refs[ring : ring + count], refs[ring + count : -1], refs[-1]
    step = pl.program_id(0)
    for s in range(ring):

        @pl.when(step == s)
        def _():
            if s < ring - count:
                out_ref[...] = data[s][...]
            else:
                out_ref[...] = data[s][...] - back[s - ring + count][...]

    if template:
        both_ref, azimuth_ref = refs[:2]
        rows = out_ref.shape[0]
        levels = dot(both_ref[...], onehot_of(azimuth_ref[...], both_ref.shape[1]))
        out_ref[...] -= levels[:rows] + levels[rows:]


def finish_piece(ring, at, start, data, back, template, azimuth, old):
    rows, width = data[0].shape
    samples = azimuth.shape[1]
    per_block, offset = BLOCK // width, start // width

    def where(s, at_ref):
        return 0, lax.rem(at_ref[0] + s, ring) * per_block + offset

    specs = [pl.BlockSpec((rows, width), lambda s, at_ref: (0, 0))] * (len(data) + len(back))
    operands = [*data, *back]
    if template is not None:
        specs += [pl.BlockSpec(template.shape, lambda s, at_ref: (0, 0)), pl.BlockSpec((1, width), where)]
        operands += [template, azimuth]
    if old is not None:
        specs += [pl.BlockSpec(memory_space=pl.ANY)]
        operands += [old]
    return pl.pallas_call(
        functools.partial(finish_kernel, ring, len(back), template is not None),
        out_shape=jax.ShapeDtypeStruct((rows, samples), jnp.float32),
        grid_spec=pltpu.PrefetchScalarGridSpec(
            num_scalar_prefetch=1,
            grid=(ring,),
            in_specs=specs,
            out_specs=pl.BlockSpec((rows, width), where),
        ),
        input_output_aliases={len(operands): 0} if old is not None else {},
        cost_estimate=pl.CostEstimate(
            flops=4 * ring * rows * width * (NBIN if template is not None else 1),
            bytes_accessed=12 * ring * rows * width,
            transcendentals=0,
        ),
    )(at, *operands)


def level_kernel(ring, start, at_ref, both_ref, azimuth_ref, back_ref, *refs):
    data, outs = refs[:ring], refs[ring:]
    rows, width = outs[0].shape
    for s in range(ring):
        azimuth = azimuth_ref[:, pl.ds(block_start(ring, at_ref[0], s, start), width)]
        levels = dot(both_ref[...], onehot_of(azimuth, both_ref.shape[1]))
        value = data[s][...] - (levels[:rows] + levels[rows:])
        outs[s][...] = value - back_ref[...] if s == 0 else value


def level_piece(ring, at, start, data, back, template, azimuth):
    rows, width = data[0].shape
    return pl.pallas_call(
        functools.partial(level_kernel, ring, start),
        out_shape=[jax.ShapeDtypeStruct((rows, width), jnp.float32)] * ring,
        in_specs=[pl.BlockSpec(memory_space=pltpu.SMEM)] + [pl.BlockSpec(memory_space=pltpu.VMEM)] * (3 + ring),
        out_specs=[pl.BlockSpec(memory_space=pltpu.VMEM)] * ring,
        cost_estimate=pl.CostEstimate(
            flops=4 * ring * rows * width * NBIN, bytes_accessed=8 * ring * rows * width, transcendentals=0
        ),
    )(at, template, azimuth, back, *data)


def exchanged_blocks(ring, shares, tod, gain_knots, intervals, fraction, azimuth, mode_index, mode_bank, mode_mix):
    det_rows, samples = tod.shape
    me = lax.axis_index("det")
    tm = lax.axis_index("tm")
    part_of = lax.axis_index("groups") * lax.axis_size("tm") + tm
    which = lax.dynamic_index_in_dim(mode_index, me, 0, False)
    me_only = jnp.full((1,), me, jnp.int32)
    at = jnp.stack([me, which, part_of, lax.rem(tm, 2), tm])

    def send(array, shift):
        return lax.ppermute(array, "det", [(i, (i + shift) % ring) for i in range(ring)])

    def swap(array, axis, bit):
        return lax.ppermute(array, axis, [(i, i ^ bit) for i in range(lax.axis_size(axis))])

    gains = gain_knots.T
    where, share = intervals[None, :], fraction[None, :]
    azimuth = azimuth[None, :]
    data, arrived = {}, {}
    order = [[(s, start, width) for s in (1, 2, 3)] for start, width in PIECES]
    order[-1] += [(0, start, width) for start, width in PIECES]
    for pieces in order:
        blocks = calibrate(ring, me_only, tod, gains, where, share, pieces)
        for (s, start, width), block in zip(pieces, blocks):
            data[s, start] = block
            arrived[s, start] = send(block, s) if s else block

    rows = det_rows // shares
    banks = lax.dynamic_slice_in_dim(mode_bank, part_of * rows, rows, 1)[None]
    for bit in (2, 1):
        banks = jnp.concatenate([banks, swap(banks, "det", bit)], axis=0)
    by_x = swap(banks, "tm", 2)
    by_y = swap(banks, "groups", 1)
    diagonal = [swap(by_x[:2], "groups", 1), swap(by_y[2:], "tm", 2)]
    banks = jnp.concatenate([banks, by_x, by_y, *diagonal], axis=0)
    banks = jnp.concatenate([banks, swap(banks, "tm", 1)], axis=0)

    pieces = [piece for part in order for piece in part]
    keep, other = bin_data(ring, at, mode_index, azimuth, pieces, [data[s, start] for s, start, _ in pieces])
    sums = keep + swap(other, "tm", 1)
    half = NBIN // 2
    sums = sums[:, :half] + swap(sums[:, half:], "tm", 2)
    mine, cross, near = pool(ring, shares, at, banks, mode_bank, mode_mix, sums)
    near = swap(near, "det", 1)
    cross = swap(cross + near[det_rows:], "det", 2)
    template = mine - near[:det_rows] - cross
    template = jnp.concatenate([template, swap(template, "tm", 2)], axis=1)
    other = swap(template, "tm", 1)

    counts = jnp.sum((lax.broadcasted_iota(jnp.int32, (NBIN, samples), 0) == azimuth).astype(jnp.float32), axis=1)
    counts = jnp.broadcast_to(counts[None, :], (8, NBIN))
    for bit in (1, 2):
        counts = counts + swap(counts, "tm", bit)
    template = stack_template(at, template, other, counts)

    modes = prepare_modes(ring, shares, at, banks, mode_mix)
    out = None
    for part, (start, width) in enumerate(PIECES):
        removed = common_mode(ring, modes, [arrived[s, start] for s in range(ring)])
        back = [send(removed[s], -s) if s else removed[s] for s in range(ring)]
        mine = [data[s, start] for s in range(ring)]
        if part == len(PIECES) - 1:
            mine = level_piece(ring, at, start, mine, back[0], template, azimuth)
            back, template = back[1:], None
        out = finish_piece(ring, at, start, mine, back, template, azimuth, out)
    return out


def solution(mesh):
    placed = (
        P(("groups", "det"), "tm"),
        P(("groups", "det"), None),
        P(("groups", "tm")),
        P(("groups", "tm")),
        P(("groups", "tm")),
        P(("groups", "tm")),
        P(None, "det", None),
        P(),
    )
    ring = mesh.shape["det"]
    shares = mesh.shape["groups"] * mesh.shape["tm"]

    def on_device(tod, gain_knots, intervals, fraction, azimuth, mode_index, mode_bank, mode_mix):
        args = (tod, gain_knots, intervals, fraction, azimuth, mode_index, mode_bank, mode_mix)
        if ring == 4 and mode_index.shape[0] == ring and shares == 8 and mesh.shape["tm"] == 4 and mode_bank.shape[0] == 2 and tod.shape[0] % (16 * shares) == 0:
            return exchanged_blocks(ring, shares, *args)
        return gathered_sums(*args)

    return jax.shard_map(
        on_device, mesh=mesh, in_specs=placed, out_specs=P(("groups", "det"), "tm"), check_vma=False
    )
```

```python
import functools
import jax
import jax.numpy as jnp
from jax import lax
from jax.experimental import pallas as pl
from jax.experimental.pallas import tpu as pltpu
from jax.sharding import PartitionSpec as P

BLOCK = 1024
NBIN = 512
PIECES = ((0, 256), (512, 512), (256, 128), (384, 128))
LATE = 2


def gathered_sums(tod, gain_knots, intervals, fraction, azimuth, mode_index, mode_bank, mode_mix):
    precise = lax.Precision.HIGHEST
    det_rows, samples = tod.shape
    knot_row = lax.broadcasted_iota(jnp.int32, (gain_knots.shape[1], samples), 0)
    spread = jnp.where(knot_row == intervals[None, :], 1.0 - fraction[None, :], 0.0)
    spread = spread + jnp.where(knot_row == intervals[None, :] + 1, fraction[None, :], 0.0)
    calibrated = tod * jnp.dot(gain_knots, spread, precision=precise)
    nblocks = samples // BLOCK
    blocks = calibrated.reshape(det_rows, nblocks, BLOCK)
    selected = jnp.take(mode_bank, mode_index, axis=0)
    mixing = jnp.take(mode_mix, mode_index, axis=0)
    partial_amps = jnp.einsum("kdm,dkt->kmt", selected, blocks, precision=precise)
    share = lax.psum_scatter(partial_amps, "det", scatter_dimension=2, tiled=True)
    coef_share = share + jnp.einsum("kmn,knt->kmt", mixing, share, precision=precise)
    coef = lax.all_gather(coef_share, "det", axis=2, tiled=True)
    removed = jnp.einsum("kdm,kmt->dkt", selected, coef, precision=precise)
    cleaned = (blocks - removed).reshape(det_rows, samples)
    onehot = (lax.broadcasted_iota(jnp.int32, (NBIN, samples), 0) == azimuth[None, :]).astype(
        tod.dtype
    )
    fit_part = lax.dot_general(cleaned, onehot, (((1,), (1,)), ((), ())), precision=precise)
    count_part = jnp.sum(onehot, axis=1)
    fit, counts = lax.psum((fit_part, count_part), "tm")
    template = fit / jnp.maximum(counts, 1.0)[None, :]
    return cleaned - jnp.dot(template, onehot, precision=precise)


def halves(x):
    high = x.astype(jnp.bfloat16)
    return high, (x - high.astype(jnp.float32)).astype(jnp.bfloat16)


def dot(a, b, contract=((1,), (0,))):
    return lax.dot_general(a, b, (contract, ((), ())), preferred_element_type=jnp.float32)


def dot3(a, b):
    return dot(a[0], b[0]) + (dot(a[0], b[1]) + dot(a[1], b[0]))


def calibrate_kernel(count, me_ref, gain_ref, *refs):
    gain_high, gain_low = halves(gain_ref[...])
    gains = jnp.concatenate([gain_high, gain_high, gain_low, gain_low], axis=0)
    knots = gain_ref.shape[0]
    for n in range(count):
        tod_ref, where_ref, share_ref = refs[3 * n : 3 * n + 3]
        knot_row = lax.broadcasted_iota(jnp.int32, (knots, tod_ref.shape[1]), 0)
        where, share = where_ref[...], share_ref[...]
        spread = jnp.where(knot_row == where, 1.0 - share, 0.0)
        spread = spread + jnp.where(knot_row == where + 1, share, 0.0)
        high, low = halves(spread)
        spreads = jnp.concatenate([high, low, high, low], axis=0)
        refs[3 * count + n][...] = tod_ref[...] * dot(gains, spreads, ((0,), (0,)))


def calibrate(ring, me, tod, gains, where, share, pieces):
    rows = tod.shape[0]
    specs, operands = [], []
    for shift, start, width in pieces:
        per_block, offset = BLOCK // width, start // width

        def at(i, me_ref, shift=shift, per_block=per_block, offset=offset):
            return 0, lax.rem(me_ref[0] + shift, ring) * per_block + offset

        specs += [pl.BlockSpec((rows, width), at)] + [pl.BlockSpec((1, width), at)] * 2
        operands += [tod, where, share]
    return pl.pallas_call(
        functools.partial(calibrate_kernel, len(pieces)),
        out_shape=[jax.ShapeDtypeStruct((rows, width), jnp.float32) for _, _, width in pieces],
        grid_spec=pltpu.PrefetchScalarGridSpec(
            num_scalar_prefetch=1,
            grid=(1,),
            in_specs=[pl.BlockSpec(gains.shape, lambda i, me_ref: (0, 0))] + specs,
            out_specs=[pl.BlockSpec((rows, width), lambda i, me_ref: (0, 0)) for _, _, width in pieces],
        ),
        cost_estimate=pl.CostEstimate(
            flops=2 * rows * 256 * sum(w for _, _, w in pieces),
            bytes_accessed=8 * rows * sum(w for _, _, w in pieces),
            transcendentals=0,
        ),
    )(me, gains, *operands)


def modes_kernel(ring, shares, at_ref, bank_ref, mix_ref, first_high, first_low, second_high, second_low, modes):
    rows = bank_ref.shape[2]
    me, part = at_ref[0], at_ref[2]
    other = jnp.bitwise_xor(me, lax.rem(me - pl.program_id(0) + ring, ring))
    z_slot = (other // 2) + 2 * lax.rem(other, 2)
    for share in range(shares):
        flip = jnp.bitwise_xor(part, share)
        slot = z_slot + ring * (lax.rem(flip // 2, 2) + 2 * (flip // 4) + 4 * lax.rem(flip, 2))
        modes[pl.ds(share * rows, rows), :] = bank_ref[slot, 0]
    u = modes[...]
    mixed = u + dot3(halves(u), halves(mix_ref[0]))
    first_high[...], first_low[...] = halves(u.T)
    second_high[...], second_low[...] = halves(mixed)


def prepare_modes(ring, shares, at, banks, mode_mix):
    _, _, rows, m = banks.shape
    det_rows = rows * shares
    first = pl.BlockSpec((m, det_rows), lambda s, at_ref: (0, s))
    second = pl.BlockSpec((det_rows, m), lambda s, at_ref: (s, 0))
    total = ring * det_rows
    return pl.pallas_call(
        functools.partial(modes_kernel, ring, shares),
        out_shape=[jax.ShapeDtypeStruct((m, total), jnp.bfloat16)] * 2
        + [jax.ShapeDtypeStruct((total, m), jnp.bfloat16)] * 2,
        grid_spec=pltpu.PrefetchScalarGridSpec(
            num_scalar_prefetch=1,
            grid=(ring,),
            in_specs=[
                pl.BlockSpec((banks.shape[0], 1, rows, m), lambda s, at_ref: (0, at_ref[1], 0, 0)),
                pl.BlockSpec((1, m, m), lambda s, at_ref: (at_ref[1], 0, 0)),
            ],
            out_specs=[first, first, second, second],
            scratch_shapes=[pltpu.VMEM((det_rows, m), jnp.float32)],
        ),
        cost_estimate=pl.CostEstimate(
            flops=6 * total * m * m, bytes_accessed=12 * total * m, transcendentals=0
        ),
    )(at, banks, mode_mix)


def filter_kernel(ring, first_high, first_low, second_high, second_low, *refs):
    rows = refs[0].shape[0]
    data = halves(jnp.concatenate([refs[s][...] for s in range(ring)], axis=0))
    amps = dot3((first_high[...], first_low[...]), data)
    amps = halves(amps)
    for s in range(ring):
        block = pl.ds(s * rows, rows)
        refs[ring + s][...] = dot3((second_high[block, :], second_low[block, :]), amps)


def common_mode(ring, modes, arrived):
    rows, width = arrived[0].shape
    m, total = modes[0].shape
    tile = min(width, 256)
    whole = [pl.BlockSpec((m, total), lambda i: (0, 0))] * 2 + [pl.BlockSpec((total, m), lambda i: (0, 0))] * 2
    column = pl.BlockSpec((rows, tile), lambda i: (0, i))
    return pl.pallas_call(
        functools.partial(filter_kernel, ring),
        out_shape=[jax.ShapeDtypeStruct((rows, width), jnp.float32)] * ring,
        grid=(width // tile,),
        in_specs=whole + [column] * ring,
        out_specs=[column] * ring,
        cost_estimate=pl.CostEstimate(
            flops=12 * total * m * width, bytes_accessed=8 * total * width, transcendentals=0
        ),
    )(*modes, *arrived)


def share_kernel(part_ref, bank_ref, out_ref):
    out_ref[0] = bank_ref[...]


def own_share(part, mode_bank, shares):
    count, rows, m = mode_bank.shape
    return pl.pallas_call(
        share_kernel,
        out_shape=jax.ShapeDtypeStruct((1, count, rows // shares, m), jnp.float32),
        grid_spec=pltpu.PrefetchScalarGridSpec(
            num_scalar_prefetch=1,
            grid=(1,),
            in_specs=[pl.BlockSpec((count, rows // shares, m), lambda i, part_ref: (0, part_ref[0], 0))],
            out_specs=pl.BlockSpec((1, count, rows // shares, m), lambda i, part_ref: (0, 0, 0, 0)),
        ),
    )(part, mode_bank)


def last_kernel(ring, start, at_ref, *refs):
    data, back = refs[:ring], refs[ring : 2 * ring - 1]
    out_ref, held, done = refs[-3:]
    copies = []
    for s in range(ring):
        held[s] = data[s][...] - back[s - 1][...] if s else data[s][...]
        column = pl.ds(block_start(ring, at_ref[0], s, start), held.shape[2])
        copies.append(pltpu.make_async_copy(held.at[s], out_ref.at[:, column], done.at[s]))
        copies[s].start()
    for copy in copies:
        copy.wait()


def last_piece(ring, at, start, data, back, old):
    rows, width = data[0].shape
    return pl.pallas_call(
        functools.partial(last_kernel, ring, start),
        out_shape=jax.ShapeDtypeStruct(old.shape, jnp.float32),
        in_specs=[pl.BlockSpec(memory_space=pltpu.SMEM)]
        + [pl.BlockSpec(memory_space=pltpu.VMEM)] * (2 * ring - 1)
        + [pl.BlockSpec(memory_space=pl.ANY)],
        out_specs=pl.BlockSpec(memory_space=pl.ANY),
        scratch_shapes=[pltpu.VMEM((ring, rows, width), jnp.float32), pltpu.SemaphoreType.DMA((ring,))],
        input_output_aliases={2 * ring: 0},
        compiler_params=pltpu.CompilerParams(vmem_limit_bytes=65_000_000),
        cost_estimate=pl.CostEstimate(
            flops=ring * rows * width, bytes_accessed=12 * ring * rows * width, transcendentals=0
        ),
    )(at, *data, *back, old)


def onehot_of(azimuth, bins):
    row = lax.broadcasted_iota(jnp.int32, (bins, azimuth.shape[1]), 0)
    return (row == azimuth).astype(jnp.float32).astype(jnp.bfloat16)


def block_start(ring, me, shift, start):
    return pl.multiple_of(lax.rem(me + shift, ring) * BLOCK + start, 128)


def bin_kernel(ring, pieces, at_ref, index_ref, azimuth_ref, *refs):
    data, (keep_ref, send_ref, sums) = refs[: len(pieces)], refs[len(pieces) :]
    me, tm = at_ref[0], at_ref[4]
    rows = keep_ref.shape[0]
    sums[...] = jnp.zeros_like(sums)
    for (shift, start, width), ref in zip(pieces, data):
        both = jnp.concatenate(halves(ref[...]), axis=0)
        onehot = onehot_of(azimuth_ref[:, pl.ds(block_start(ring, me, shift, start), width)], sums.shape[2])
        part = dot(both, onehot, ((1,), (1,)))
        sums[index_ref[lax.rem(me + shift, ring)]] += part[:rows] + part[rows:]
    share = sums.shape[2] // 4
    for x in range(2):
        for bank in range(2):
            column = slice((2 * x + bank) * share, (2 * x + bank + 1) * share)
            for flip, ref in ((0, keep_ref), (1, send_ref)):
                first = pl.multiple_of(jnp.bitwise_xor(tm, 2 * x + flip) * share, share)
                ref[:, column] = sums[bank, :, pl.ds(first, share)]


def bin_data(ring, at, mode_index, azimuth, pieces, data):
    rows = data[0].shape[0]
    work = sum(width for _, _, width in pieces)
    return pl.pallas_call(
        functools.partial(bin_kernel, ring, pieces),
        out_shape=[jax.ShapeDtypeStruct((rows, NBIN), jnp.float32)] * 2,
        in_specs=[pl.BlockSpec(memory_space=pltpu.SMEM)] * 2 + [pl.BlockSpec(memory_space=pltpu.VMEM)] * (1 + len(data)),
        out_specs=[pl.BlockSpec(memory_space=pltpu.VMEM)] * 2,
        scratch_shapes=[pltpu.VMEM((2, rows, NBIN), jnp.float32)],
        cost_estimate=pl.CostEstimate(
            flops=4 * rows * work * NBIN, bytes_accessed=4 * rows * work, transcendentals=0
        ),
    )(at, mode_index, azimuth, *data)


def pool_kernel(ring, shares, at_ref, bank_ref, own_ref, mix_ref, sums_ref, mine_ref, cross_ref, near_ref, total):
    step = pl.program_id(0)
    slots, _, rows, m = bank_ref.shape
    sums = halves(sums_ref[...])
    amps = [halves(own_ref[0].T)[n] for n in range(2)]
    amps = dot3(amps, sums)
    coef = halves(amps + dot3(halves(mix_ref[0]), halves(amps)))
    removed = dot3(halves(bank_ref[:, 0].reshape(slots * rows, m)), coef)

    @pl.when(step == 0)
    def _():
        total[...] = removed
        mine_ref[...] = sums_ref[...]

    @pl.when(step == 1)
    def _():
        total[...] += removed
        mine_ref[...] += sums_ref[...]
        part = at_ref[2]
        for p in range(shares):
            flip = jnp.bitwise_xor(part, p)
            slot = ring * (lax.rem(flip // 2, 2) + 2 * (flip // 4) + 4 * lax.rem(flip, 2))
            block = slice(p * rows, (p + 1) * rows)

            def rows_of(z):
                return total[pl.ds(pl.multiple_of((slot + z) * rows, rows), rows), :]

            mine_ref[block, :] -= rows_of(0)
            cross_ref[block, :] = rows_of(1)
            near_ref[block, :] = rows_of(2)
            near_ref[p * rows + shares * rows : (p + 1) * rows + shares * rows, :] = rows_of(3)


def pool(ring, shares, at, banks, mode_bank, mode_mix, sums):
    slots, _, rows, m = banks.shape
    det_rows, share = rows * shares, sums.shape[1] // 2
    shapes = [(det_rows, share), (det_rows, share), (2 * det_rows, share)]
    return pl.pallas_call(
        functools.partial(pool_kernel, ring, shares),
        out_shape=[jax.ShapeDtypeStruct(shape, jnp.float32) for shape in shapes],
        grid_spec=pltpu.PrefetchScalarGridSpec(
            num_scalar_prefetch=1,
            grid=(2,),
            in_specs=[
                pl.BlockSpec((slots, 1, rows, m), lambda b, at_ref: (0, b, 0, 0)),
                pl.BlockSpec((1, det_rows, m), lambda b, at_ref: (b, 0, 0)),
                pl.BlockSpec((1, m, m), lambda b, at_ref: (b, 0, 0)),
                pl.BlockSpec((det_rows, share), lambda b, at_ref: (0, b)),
            ],
            out_specs=[pl.BlockSpec(shape, lambda b, at_ref: (0, 0)) for shape in shapes],
            scratch_shapes=[pltpu.VMEM((slots * rows, share), jnp.float32)],
        ),
        cost_estimate=pl.CostEstimate(
            flops=30 * slots * rows * m * share, bytes_accessed=8 * slots * rows * m, transcendentals=0
        ),
    )(at, banks, mode_bank, mode_mix, sums)


def stack_kernel(at_ref, here_ref, there_ref, counts_ref, both_ref):
    tm = at_ref[4]
    rows, width = here_ref.shape
    share = width // 2
    for flip, ref in ((0, here_ref), (1, there_ref)):
        for x in range(2):
            first = pl.multiple_of(jnp.bitwise_xor(tm, 2 * x + flip) * share, share)
            counts = jnp.maximum(counts_ref[:1, pl.ds(first, share)], 1.0)
            high, low = halves(ref[:, x * share : (x + 1) * share] / counts)
            both_ref[:rows, pl.ds(first, share)] = high
            both_ref[rows:, pl.ds(first, share)] = low


def stack_template(at, here, there, counts):
    return pl.pallas_call(
        stack_kernel,
        out_shape=jax.ShapeDtypeStruct((2 * here.shape[0], NBIN), jnp.bfloat16),
        in_specs=[pl.BlockSpec(memory_space=pltpu.SMEM)] + [pl.BlockSpec(memory_space=pltpu.VMEM)] * 3,
        out_specs=pl.BlockSpec(memory_space=pltpu.VMEM),
    )(at, here, there, counts)


def finish_kernel(ring, at_ref, *refs):
    data, back = refs[:ring], refs[ring : 2 * ring]
    both_ref, azimuth_ref = refs[2 * ring : 2 * ring + 2]
    out_ref = refs[-1]
    rows = out_ref.shape[0]
    levels = dot(both_ref[...], onehot_of(azimuth_ref[...], both_ref.shape[1]))
    levels = levels[:rows] + levels[rows:]
    for s in range(ring):

        @pl.when(pl.program_id(0) == s)
        def _():
            out_ref[...] = data[s][...] - back[s][...] - levels


def finish_piece(ring, at, start, data, back, template, azimuth, old):
    rows, width = data[0].shape
    samples = azimuth.shape[1]
    per_block, offset = BLOCK // width, start // width

    def where(s, at_ref):
        return 0, lax.rem(at_ref[0] + s, ring) * per_block + offset

    operands = [*data, *back, template, azimuth]
    specs = [pl.BlockSpec((rows, width), lambda s, at_ref: (0, 0))] * (2 * ring)
    specs += [pl.BlockSpec(template.shape, lambda s, at_ref: (0, 0)), pl.BlockSpec((1, width), where)]
    if old is not None:
        specs += [pl.BlockSpec(memory_space=pl.ANY)]
        operands += [old]
    return pl.pallas_call(
        functools.partial(finish_kernel, ring),
        out_shape=jax.ShapeDtypeStruct((rows, samples), jnp.float32),
        grid_spec=pltpu.PrefetchScalarGridSpec(
            num_scalar_prefetch=1,
            grid=(ring,),
            in_specs=specs,
            out_specs=pl.BlockSpec((rows, width), where),
        ),
        input_output_aliases={len(operands): 0} if old is not None else {},
        cost_estimate=pl.CostEstimate(
            flops=4 * ring * rows * width * NBIN, bytes_accessed=12 * ring * rows * width, transcendentals=0
        ),
    )(at, *operands)


def level_kernel(ring, start, at_ref, both_ref, azimuth_ref, back_ref, *refs):
    data, outs = refs[:ring], refs[ring:]
    rows, width = outs[0].shape
    for s in range(ring):
        azimuth = azimuth_ref[:, pl.ds(block_start(ring, at_ref[0], s, start), width)]
        levels = dot(both_ref[...], onehot_of(azimuth, both_ref.shape[1]))
        value = data[s][...] - (levels[:rows] + levels[rows:])
        outs[s][...] = value - back_ref[...] if s == 0 else value


def level_piece(ring, at, start, data, back, template, azimuth):
    rows, width = data[0].shape
    return pl.pallas_call(
        functools.partial(level_kernel, ring, start),
        out_shape=[jax.ShapeDtypeStruct((rows, width), jnp.float32)] * ring,
        in_specs=[pl.BlockSpec(memory_space=pltpu.SMEM)] + [pl.BlockSpec(memory_space=pltpu.VMEM)] * (3 + ring),
        out_specs=[pl.BlockSpec(memory_space=pltpu.VMEM)] * ring,
        cost_estimate=pl.CostEstimate(
            flops=4 * ring * rows * width * NBIN, bytes_accessed=8 * ring * rows * width, transcendentals=0
        ),
    )(at, template, azimuth, back, *data)


def exchanged_blocks(ring, shares, tod, gain_knots, intervals, fraction, azimuth, mode_index, mode_bank, mode_mix):
    det_rows, samples = tod.shape
    me = lax.axis_index("det")
    tm = lax.axis_index("tm")
    part_of = lax.axis_index("groups") * lax.axis_size("tm") + tm
    which = lax.dynamic_index_in_dim(mode_index, me, 0, False)
    me_only = jnp.full((1,), me, jnp.int32)
    at = jnp.stack([me, which, part_of, lax.rem(tm, 2), tm])

    def send(array, shift):
        return lax.ppermute(array, "det", [(i, (i + shift) % ring) for i in range(ring)])

    def swap(array, axis, bit):
        return lax.ppermute(array, axis, [(i, i ^ bit) for i in range(lax.axis_size(axis))])

    gains = gain_knots.T
    where, share = intervals[None, :], fraction[None, :]
    azimuth = azimuth[None, :]
    data, arrived = {}, {}
    order = [[(s, start, width) for s in (1, 2, 3)] for start, width in PIECES]
    order[-1] += [(0, start, width) for start, width in PIECES]
    for pieces in order:
        blocks = calibrate(ring, me_only, tod, gains, where, share, pieces)
        for (s, start, width), block in zip(pieces, blocks):
            data[s, start] = block
            arrived[s, start] = send(block, s) if s else block

    banks = own_share(jnp.full((1,), part_of, jnp.int32), mode_bank, shares)
    for bit in (2, 1):
        banks = jnp.concatenate([banks, swap(banks, "det", bit)], axis=0)
    by_x = swap(banks, "tm", 2)
    by_y = swap(banks, "groups", 1)
    diagonal = [swap(by_x[:2], "groups", 1), swap(by_y[2:], "tm", 2)]
    banks = jnp.concatenate([banks, by_x, by_y, *diagonal], axis=0)
    banks = jnp.concatenate([banks, swap(banks, "tm", 1)], axis=0)

    pieces = [piece for part in order for piece in part]
    keep, other = bin_data(ring, at, mode_index, azimuth, pieces, [data[s, start] for s, start, _ in pieces])
    sums = keep + swap(other, "tm", 1)
    half = NBIN // 2
    sums = sums[:, :half] + swap(sums[:, half:], "tm", 2)
    mine, cross, near = pool(ring, shares, at, banks, mode_bank, mode_mix, sums)
    near = swap(near, "det", 1)
    cross = swap(cross + near[det_rows:], "det", 2)
    template = mine - near[:det_rows] - cross
    template = jnp.concatenate([template, swap(template, "tm", 2)], axis=1)
    other = swap(template, "tm", 1)

    counts = jnp.sum((lax.broadcasted_iota(jnp.int32, (NBIN, samples), 0) == azimuth).astype(jnp.float32), axis=1)
    counts = jnp.broadcast_to(counts[None, :], (8, NBIN))
    for bit in (1, 2):
        counts = counts + swap(counts, "tm", bit)
    template = stack_template(at, template, other, counts)

    modes = prepare_modes(ring, shares, at, banks, mode_mix)
    out = None
    for part, (start, width) in enumerate(PIECES):
        removed = common_mode(ring, modes, [arrived[s, start] for s in range(ring)])
        back = [send(removed[s], -s) if s else removed[s] for s in range(ring)]
        mine = [data[s, start] for s in range(ring)]
        if part < len(PIECES) - LATE:
            out = finish_piece(ring, at, start, mine, back, template, azimuth, out)
        else:
            mine = level_piece(ring, at, start, mine, back[0], template, azimuth)
            out = last_piece(ring, at, start, mine, back[1:], out)
    return out


def solution(mesh):
    placed = (
        P(("groups", "det"), "tm"),
        P(("groups", "det"), None),
        P(("groups", "tm")),
        P(("groups", "tm")),
        P(("groups", "tm")),
        P(("groups", "tm")),
        P(None, "det", None),
        P(),
    )
    ring = mesh.shape["det"]
    shares = mesh.shape["groups"] * mesh.shape["tm"]

    def on_device(tod, gain_knots, intervals, fraction, azimuth, mode_index, mode_bank, mode_mix):
        args = (tod, gain_knots, intervals, fraction, azimuth, mode_index, mode_bank, mode_mix)
        if ring == 4 and mode_index.shape[0] == ring and shares == 8 and mesh.shape["tm"] == 4 and mode_bank.shape[0] == 2 and tod.shape[0] % (16 * shares) == 0:
            return exchanged_blocks(ring, shares, *args)
        return gathered_sums(*args)

    return jax.shard_map(
        on_device, mesh=mesh, in_specs=placed, out_specs=P(("groups", "det"), "tm"), check_vma=False
    )
```

```python
import functools
import jax
import jax.numpy as jnp
from jax import lax
from jax.experimental import pallas as pl
from jax.experimental.pallas import tpu as pltpu
from jax.sharding import PartitionSpec as P

BLOCK = 1024
NBIN = 512
PIECES = ((0, 256), (512, 512), (256, 128), (384, 128))
LATE = 2
GRANT = pltpu.CompilerParams(vmem_limit_bytes=32 * 1024 * 1024)


def gathered_sums(tod, gain_knots, intervals, fraction, azimuth, mode_index, mode_bank, mode_mix):
    precise = lax.Precision.HIGHEST
    det_rows, samples = tod.shape
    knot_row = lax.broadcasted_iota(jnp.int32, (gain_knots.shape[1], samples), 0)
    spread = jnp.where(knot_row == intervals[None, :], 1.0 - fraction[None, :], 0.0)
    spread = spread + jnp.where(knot_row == intervals[None, :] + 1, fraction[None, :], 0.0)
    calibrated = tod * jnp.dot(gain_knots, spread, precision=precise)
    nblocks = samples // BLOCK
    blocks = calibrated.reshape(det_rows, nblocks, BLOCK)
    selected = jnp.take(mode_bank, mode_index, axis=0)
    mixing = jnp.take(mode_mix, mode_index, axis=0)
    partial_amps = jnp.einsum("kdm,dkt->kmt", selected, blocks, precision=precise)
    share = lax.psum_scatter(partial_amps, "det", scatter_dimension=2, tiled=True)
    coef_share = share + jnp.einsum("kmn,knt->kmt", mixing, share, precision=precise)
    coef = lax.all_gather(coef_share, "det", axis=2, tiled=True)
    removed = jnp.einsum("kdm,kmt->dkt", selected, coef, precision=precise)
    cleaned = (blocks - removed).reshape(det_rows, samples)
    onehot = (lax.broadcasted_iota(jnp.int32, (NBIN, samples), 0) == azimuth[None, :]).astype(
        tod.dtype
    )
    fit_part = lax.dot_general(cleaned, onehot, (((1,), (1,)), ((), ())), precision=precise)
    count_part = jnp.sum(onehot, axis=1)
    fit, counts = lax.psum((fit_part, count_part), "tm")
    template = fit / jnp.maximum(counts, 1.0)[None, :]
    return cleaned - jnp.dot(template, onehot, precision=precise)


def halves(x):
    high = x.astype(jnp.bfloat16)
    return high, (x - high.astype(jnp.float32)).astype(jnp.bfloat16)


def dot(a, b, contract=((1,), (0,))):
    return lax.dot_general(a, b, (contract, ((), ())), preferred_element_type=jnp.float32)


def dot3(a, b):
    return dot(a[0], b[0]) + (dot(a[0], b[1]) + dot(a[1], b[0]))


def calibrate_kernel(count, me_ref, gain_ref, *refs):
    gain_high, gain_low = halves(gain_ref[...])
    gains = jnp.concatenate([gain_high, gain_high, gain_low, gain_low], axis=0)
    knots = gain_ref.shape[0]
    for n in range(count):
        tod_ref, where_ref, share_ref = refs[3 * n : 3 * n + 3]
        knot_row = lax.broadcasted_iota(jnp.int32, (knots, tod_ref.shape[1]), 0)
        where, share = where_ref[...], share_ref[...]
        spread = jnp.where(knot_row == where, 1.0 - share, 0.0)
        spread = spread + jnp.where(knot_row == where + 1, share, 0.0)
        high, low = halves(spread)
        spreads = jnp.concatenate([high, low, high, low], axis=0)
        refs[3 * count + n][...] = tod_ref[...] * dot(gains, spreads, ((0,), (0,)))


def calibrate(me, tod, gains, where, share, pieces, grant, place):
    rows = tod.shape[0]
    specs, operands = [], []
    for shift, start, width in pieces:
        per_block, offset = BLOCK // width, start // width

        def at(i, me_ref, shift=shift, per_block=per_block, offset=offset):
            return 0, jnp.bitwise_xor(me_ref[0], shift) * per_block + offset

        specs += [pl.BlockSpec((rows, width), at)] + [pl.BlockSpec((1, width), at)] * 2
        operands += [tod, where, share]
    return pl.pallas_call(
        functools.partial(calibrate_kernel, len(pieces)),
        compiler_params=grant,
        out_shape=[place((rows, width), jnp.float32) for _, _, width in pieces],
        grid_spec=pltpu.PrefetchScalarGridSpec(
            num_scalar_prefetch=1,
            grid=(1,),
            in_specs=[pl.BlockSpec(gains.shape, lambda i, me_ref: (0, 0))] + specs,
            out_specs=[pl.BlockSpec((rows, width), lambda i, me_ref: (0, 0)) for _, _, width in pieces],
        ),
        cost_estimate=pl.CostEstimate(
            flops=2 * rows * 256 * sum(w for _, _, w in pieces),
            bytes_accessed=8 * rows * sum(w for _, _, w in pieces),
            transcendentals=0,
        ),
    )(me, gains, *operands)


def modes_kernel(ring, shares, at_ref, bank_ref, mix_ref, first_high, first_low, second_high, second_low, modes):
    rows = bank_ref.shape[2]
    part = at_ref[2]
    other = pl.program_id(0)
    z_slot = (other // 2) + 2 * lax.rem(other, 2)
    for share in range(shares):
        flip = jnp.bitwise_xor(part, share)
        slot = z_slot + ring * (lax.rem(flip // 2, 2) + 2 * (flip // 4) + 4 * lax.rem(flip, 2))
        modes[pl.ds(share * rows, rows), :] = bank_ref[slot, 0]
    u = modes[...]
    mixed = u + dot3(halves(u), halves(mix_ref[0]))
    first_high[...], first_low[...] = halves(u.T)
    second_high[...], second_low[...] = halves(mixed)


def prepare_modes(ring, shares, at, banks, mode_mix):
    _, _, rows, m = banks.shape
    det_rows = rows * shares
    first = pl.BlockSpec((m, det_rows), lambda s, at_ref: (0, s))
    second = pl.BlockSpec((det_rows, m), lambda s, at_ref: (s, 0))
    total = ring * det_rows
    return pl.pallas_call(
        functools.partial(modes_kernel, ring, shares),
        compiler_params=GRANT,
        out_shape=[jax.ShapeDtypeStruct((m, total), jnp.bfloat16)] * 2
        + [jax.ShapeDtypeStruct((total, m), jnp.bfloat16)] * 2,
        grid_spec=pltpu.PrefetchScalarGridSpec(
            num_scalar_prefetch=1,
            grid=(ring,),
            in_specs=[
                pl.BlockSpec((banks.shape[0], 1, rows, m), lambda s, at_ref: (0, at_ref[1], 0, 0)),
                pl.BlockSpec((1, m, m), lambda s, at_ref: (at_ref[1], 0, 0)),
            ],
            out_specs=[first, first, second, second],
            scratch_shapes=[pltpu.VMEM((det_rows, m), jnp.float32)],
        ),
        cost_estimate=pl.CostEstimate(
            flops=6 * total * m * m, bytes_accessed=12 * total * m, transcendentals=0
        ),
    )(at, banks, mode_mix)


def filter_kernel(ring, first_high, first_low, second_high, second_low, *refs):
    rows = refs[0].shape[0]
    data = halves(jnp.concatenate([refs[s][...] for s in range(ring)], axis=0))
    amps = dot3((first_high[...], first_low[...]), data)
    amps = halves(amps)
    for s in range(ring):
        block = pl.ds(s * rows, rows)
        refs[ring + s][...] = dot3((second_high[block, :], second_low[block, :]), amps)


def common_mode(ring, modes, arrived):
    rows, width = arrived[0].shape
    m, total = modes[0].shape
    tile = min(width, 256)
    whole = [pl.BlockSpec((m, total), lambda i: (0, 0))] * 2 + [pl.BlockSpec((total, m), lambda i: (0, 0))] * 2
    column = pl.BlockSpec((rows, tile), lambda i: (0, i))
    return pl.pallas_call(
        functools.partial(filter_kernel, ring),
        compiler_params=GRANT,
        out_shape=[jax.ShapeDtypeStruct((rows, width), jnp.float32)] * ring,
        grid=(width // tile,),
        in_specs=whole + [column] * ring,
        out_specs=[column] * ring,
        cost_estimate=pl.CostEstimate(
            flops=12 * total * m * width, bytes_accessed=8 * total * width, transcendentals=0
        ),
    )(*modes, *arrived)


def share_kernel(part_ref, bank_ref, out_ref):
    out_ref[0] = bank_ref[...]


def own_share(part, mode_bank, shares):
    count, rows, m = mode_bank.shape
    return pl.pallas_call(
        share_kernel,
        out_shape=pltpu.VMEM((1, count, rows // shares, m), jnp.float32),
        grid_spec=pltpu.PrefetchScalarGridSpec(
            num_scalar_prefetch=1,
            grid=(1,),
            in_specs=[pl.BlockSpec((count, rows // shares, m), lambda i, part_ref: (0, part_ref[0], 0))],
            out_specs=pl.BlockSpec((1, count, rows // shares, m), lambda i, part_ref: (0, 0, 0, 0)),
        ),
    )(part, mode_bank)


def last_kernel(ring, start, at_ref, *refs):
    data, back = refs[:ring], refs[ring : 2 * ring - 1]
    out_ref, held, done = refs[-3:]
    copies = []
    for s in range(ring):
        held[s] = data[s][...] - back[s - 1][...] if s else data[s][...]
        column = pl.ds(block_start(at_ref[0], s, start), held.shape[2])
        copies.append(pltpu.make_async_copy(held.at[s], out_ref.at[:, column], done.at[s]))
        copies[s].start()
    for copy in copies:
        copy.wait()


def last_piece(ring, at, start, data, back, old):
    rows, width = data[0].shape
    return pl.pallas_call(
        functools.partial(last_kernel, ring, start),
        out_shape=jax.ShapeDtypeStruct(old.shape, jnp.float32),
        in_specs=[pl.BlockSpec(memory_space=pltpu.SMEM)]
        + [pl.BlockSpec(memory_space=pltpu.VMEM)] * (2 * ring - 1)
        + [pl.BlockSpec(memory_space=pl.ANY)],
        out_specs=pl.BlockSpec(memory_space=pl.ANY),
        scratch_shapes=[pltpu.VMEM((ring, rows, width), jnp.float32), pltpu.SemaphoreType.DMA((ring,))],
        input_output_aliases={2 * ring: 0},
        compiler_params=GRANT,
        cost_estimate=pl.CostEstimate(
            flops=ring * rows * width, bytes_accessed=12 * ring * rows * width, transcendentals=0
        ),
    )(at, *data, *back, old)


def onehot_of(azimuth, bins):
    row = lax.broadcasted_iota(jnp.int32, (bins, azimuth.shape[1]), 0)
    return (row == azimuth).astype(jnp.float32).astype(jnp.bfloat16)


def block_start(me, shift, start):
    return pl.multiple_of(jnp.bitwise_xor(me, shift) * BLOCK + start, 128)


def bin_kernel(pieces, at_ref, index_ref, azimuth_ref, *refs):
    data, (keep_ref, send_ref, sums) = refs[: len(pieces)], refs[len(pieces) :]
    me, tm = at_ref[0], at_ref[4]
    rows = keep_ref.shape[0]
    sums[...] = jnp.zeros_like(sums)
    for (shift, start, width), ref in zip(pieces, data):
        both = jnp.concatenate(halves(ref[...]), axis=0)
        onehot = onehot_of(azimuth_ref[:, pl.ds(block_start(me, shift, start), width)], sums.shape[2])
        part = dot(both, onehot, ((1,), (1,)))
        sums[index_ref[jnp.bitwise_xor(me, shift)]] += part[:rows] + part[rows:]
    share = sums.shape[2] // 4
    for x in range(2):
        for bank in range(2):
            column = slice((2 * x + bank) * share, (2 * x + bank + 1) * share)
            for flip, ref in ((0, keep_ref), (1, send_ref)):
                first = pl.multiple_of(jnp.bitwise_xor(tm, 2 * x + flip) * share, share)
                ref[:, column] = sums[bank, :, pl.ds(first, share)]


def bin_data(at, mode_index, azimuth, pieces, data):
    rows = data[0].shape[0]
    work = sum(width for _, _, width in pieces)
    return pl.pallas_call(
        functools.partial(bin_kernel, pieces),
        compiler_params=GRANT,
        out_shape=[jax.ShapeDtypeStruct((rows, NBIN), jnp.float32)] * 2,
        in_specs=[pl.BlockSpec(memory_space=pltpu.SMEM)] * 2 + [pl.BlockSpec(memory_space=pltpu.VMEM)] * (1 + len(data)),
        out_specs=[pl.BlockSpec(memory_space=pltpu.VMEM)] * 2,
        scratch_shapes=[pltpu.VMEM((2, rows, NBIN), jnp.float32)],
        cost_estimate=pl.CostEstimate(
            flops=4 * rows * work * NBIN, bytes_accessed=4 * rows * work, transcendentals=0
        ),
    )(at, mode_index, azimuth, *data)


def pool_kernel(ring, shares, at_ref, bank_ref, own_ref, mix_ref, sums_ref, mine_ref, cross_ref, near_ref, total):
    step = pl.program_id(0)
    slots, _, rows, m = bank_ref.shape
    sums = halves(sums_ref[...])
    amps = [halves(own_ref[0].T)[n] for n in range(2)]
    amps = dot3(amps, sums)
    coef = halves(amps + dot3(halves(mix_ref[0]), halves(amps)))
    removed = dot3(halves(bank_ref[:, 0].reshape(slots * rows, m)), coef)

    @pl.when(step == 0)
    def _():
        total[...] = removed
        mine_ref[...] = sums_ref[...]

    @pl.when(step == 1)
    def _():
        total[...] += removed
        mine_ref[...] += sums_ref[...]
        part = at_ref[2]
        for p in range(shares):
            flip = jnp.bitwise_xor(part, p)
            slot = ring * (lax.rem(flip // 2, 2) + 2 * (flip // 4) + 4 * lax.rem(flip, 2))
            block = slice(p * rows, (p + 1) * rows)

            def rows_of(z):
                return total[pl.ds(pl.multiple_of((slot + z) * rows, rows), rows), :]

            mine_ref[block, :] -= rows_of(0)
            cross_ref[block, :] = rows_of(1)
            near_ref[block, :] = rows_of(2)
            near_ref[p * rows + shares * rows : (p + 1) * rows + shares * rows, :] = rows_of(3)


def pool(ring, shares, at, banks, mode_bank, mode_mix, sums):
    slots, _, rows, m = banks.shape
    det_rows, share = rows * shares, sums.shape[1] // 2
    shapes = [(det_rows, share), (det_rows, share), (2 * det_rows, share)]
    return pl.pallas_call(
        functools.partial(pool_kernel, ring, shares),
        compiler_params=GRANT,
        out_shape=[jax.ShapeDtypeStruct(shape, jnp.float32) for shape in shapes],
        grid_spec=pltpu.PrefetchScalarGridSpec(
            num_scalar_prefetch=1,
            grid=(2,),
            in_specs=[
                pl.BlockSpec((slots, 1, rows, m), lambda b, at_ref: (0, b, 0, 0)),
                pl.BlockSpec((1, det_rows, m), lambda b, at_ref: (b, 0, 0)),
                pl.BlockSpec((1, m, m), lambda b, at_ref: (b, 0, 0)),
                pl.BlockSpec((det_rows, share), lambda b, at_ref: (0, b)),
            ],
            out_specs=[pl.BlockSpec(shape, lambda b, at_ref: (0, 0)) for shape in shapes],
            scratch_shapes=[pltpu.VMEM((slots * rows, share), jnp.float32)],
        ),
        cost_estimate=pl.CostEstimate(
            flops=30 * slots * rows * m * share, bytes_accessed=8 * slots * rows * m, transcendentals=0
        ),
    )(at, banks, mode_bank, mode_mix, sums)


def stack_kernel(at_ref, here_ref, there_ref, counts_ref, both_ref):
    tm = at_ref[4]
    rows, width = here_ref.shape
    share = width // 2
    for flip, ref in ((0, here_ref), (1, there_ref)):
        for x in range(2):
            first = pl.multiple_of(jnp.bitwise_xor(tm, 2 * x + flip) * share, share)
            counts = jnp.maximum(counts_ref[:1, pl.ds(first, share)], 1.0)
            high, low = halves(ref[:, x * share : (x + 1) * share] / counts)
            both_ref[:rows, pl.ds(first, share)] = high
            both_ref[rows:, pl.ds(first, share)] = low


def stack_template(at, here, there, counts):
    return pl.pallas_call(
        stack_kernel,
        compiler_params=GRANT,
        out_shape=jax.ShapeDtypeStruct((2 * here.shape[0], NBIN), jnp.bfloat16),
        in_specs=[pl.BlockSpec(memory_space=pltpu.SMEM)] + [pl.BlockSpec(memory_space=pltpu.VMEM)] * 3,
        out_specs=pl.BlockSpec(memory_space=pltpu.VMEM),
    )(at, here, there, counts)


def finish_kernel(ring, at_ref, *refs):
    data, back = refs[:ring], refs[ring : 2 * ring]
    both_ref, azimuth_ref = refs[2 * ring : 2 * ring + 2]
    out_ref = refs[-1]
    rows = out_ref.shape[0]
    levels = dot(both_ref[...], onehot_of(azimuth_ref[...], both_ref.shape[1]))
    levels = levels[:rows] + levels[rows:]
    for s in range(ring):

        @pl.when(pl.program_id(0) == s)
        def _():
            out_ref[...] = data[s][...] - back[s][...] - levels


def finish_piece(ring, at, start, data, back, template, azimuth, old):
    rows, width = data[0].shape
    samples = azimuth.shape[1]
    per_block, offset = BLOCK // width, start // width

    def where(s, at_ref):
        return 0, jnp.bitwise_xor(at_ref[0], s) * per_block + offset

    operands = [*data, *back, template, azimuth]
    specs = [pl.BlockSpec((rows, width), lambda s, at_ref: (0, 0))] * (2 * ring)
    specs += [pl.BlockSpec(template.shape, lambda s, at_ref: (0, 0)), pl.BlockSpec((1, width), where)]
    if old is not None:
        specs += [pl.BlockSpec(memory_space=pl.ANY)]
        operands += [old]
    return pl.pallas_call(
        functools.partial(finish_kernel, ring),
        compiler_params=GRANT,
        out_shape=jax.ShapeDtypeStruct((rows, samples), jnp.float32),
        grid_spec=pltpu.PrefetchScalarGridSpec(
            num_scalar_prefetch=1,
            grid=(ring,),
            in_specs=specs,
            out_specs=pl.BlockSpec((rows, width), where),
        ),
        input_output_aliases={len(operands): 0} if old is not None else {},
        cost_estimate=pl.CostEstimate(
            flops=4 * ring * rows * width * NBIN, bytes_accessed=12 * ring * rows * width, transcendentals=0
        ),
    )(at, *operands)


def level_kernel(ring, start, at_ref, both_ref, azimuth_ref, back_ref, *refs):
    data, outs = refs[:ring], refs[ring:]
    rows, width = outs[0].shape
    for s in range(ring):
        azimuth = azimuth_ref[:, pl.ds(block_start(at_ref[0], s, start), width)]
        levels = dot(both_ref[...], onehot_of(azimuth, both_ref.shape[1]))
        value = data[s][...] - (levels[:rows] + levels[rows:])
        outs[s][...] = value - back_ref[...] if s == 0 else value


def level_piece(ring, at, start, data, back, template, azimuth):
    rows, width = data[0].shape
    return pl.pallas_call(
        functools.partial(level_kernel, ring, start),
        compiler_params=GRANT,
        out_shape=[jax.ShapeDtypeStruct((rows, width), jnp.float32)] * ring,
        in_specs=[pl.BlockSpec(memory_space=pltpu.SMEM)] + [pl.BlockSpec(memory_space=pltpu.VMEM)] * (3 + ring),
        out_specs=[pl.BlockSpec(memory_space=pltpu.VMEM)] * ring,
        cost_estimate=pl.CostEstimate(
            flops=4 * ring * rows * width * NBIN, bytes_accessed=8 * ring * rows * width, transcendentals=0
        ),
    )(at, template, azimuth, back, *data)


def exchanged_blocks(ring, shares, tod, gain_knots, intervals, fraction, azimuth, mode_index, mode_bank, mode_mix):
    det_rows, samples = tod.shape
    me = lax.axis_index("det")
    tm = lax.axis_index("tm")
    part_of = lax.axis_index("groups") * lax.axis_size("tm") + tm
    which = lax.dynamic_index_in_dim(mode_index, me, 0, False)
    me_only = jnp.full((1,), me, jnp.int32)
    at = jnp.stack([me, which, part_of, lax.rem(tm, 2), tm])

    def swap(array, axis, bit):
        return lax.ppermute(array, axis, [(i, i ^ bit) for i in range(lax.axis_size(axis))])

    gains = gain_knots.T
    where, share = intervals[None, :], fraction[None, :]
    azimuth = azimuth[None, :]
    data, arrived = {}, {}
    order = [[(s, start, width) for s in (1, 2, 3)] for start, width in PIECES]
    order[-1] += [(0, start, width) for start, width in PIECES]
    for part, pieces in enumerate(order):
        grant = GRANT if part else pltpu.CompilerParams()
        place = jax.ShapeDtypeStruct if part else pltpu.VMEM
        blocks = calibrate(me_only, tod, gains, where, share, pieces, grant, place)
        for (s, start, width), block in zip(pieces, blocks):
            data[s, start] = block
            arrived[s, start] = swap(block, "det", s) if s else block

    banks = own_share(jnp.full((1,), part_of, jnp.int32), mode_bank, shares)
    for bit in (2, 1):
        banks = jnp.concatenate([banks, swap(banks, "det", bit)], axis=0)
    by_x = swap(banks, "tm", 2)
    by_y = swap(banks, "groups", 1)
    diagonal = [swap(by_x[:2], "groups", 1), swap(by_y[2:], "tm", 2)]
    banks = jnp.concatenate([banks, by_x, by_y, *diagonal], axis=0)
    banks = jnp.concatenate([banks, swap(banks, "tm", 1)], axis=0)

    pieces = [piece for part in order for piece in part]
    keep, other = bin_data(at, mode_index, azimuth, pieces, [data[s, start] for s, start, _ in pieces])
    sums = keep + swap(other, "tm", 1)
    half = NBIN // 2
    sums = sums[:, :half] + swap(sums[:, half:], "tm", 2)
    mine, cross, near = pool(ring, shares, at, banks, mode_bank, mode_mix, sums)
    near = swap(near, "det", 1)
    cross = swap(cross + near[det_rows:], "det", 2)
    template = mine - near[:det_rows] - cross
    template = jnp.concatenate([template, swap(template, "tm", 2)], axis=1)
    other = swap(template, "tm", 1)

    counts = jnp.sum((lax.broadcasted_iota(jnp.int32, (NBIN, samples), 0) == azimuth).astype(jnp.float32), axis=1)
    counts = jnp.broadcast_to(counts[None, :], (8, NBIN))
    for bit in (1, 2):
        counts = counts + swap(counts, "tm", bit)
    template = stack_template(at, template, other, counts)

    modes = prepare_modes(ring, shares, at, banks, mode_mix)
    out = None
    for part, (start, width) in enumerate(PIECES):
        removed = common_mode(ring, modes, [arrived[s, start] for s in range(ring)])
        back = [swap(removed[s], "det", s) if s else removed[s] for s in range(ring)]
        mine = [data[s, start] for s in range(ring)]
        if part < len(PIECES) - LATE:
            out = finish_piece(ring, at, start, mine, back, template, azimuth, out)
        else:
            mine = level_piece(ring, at, start, mine, back[0], template, azimuth)
            out = last_piece(ring, at, start, mine, back[1:], out)
    return out


def solution(mesh):
    placed = (
        P(("groups", "det"), "tm"),
        P(("groups", "det"), None),
        P(("groups", "tm")),
        P(("groups", "tm")),
        P(("groups", "tm")),
        P(("groups", "tm")),
        P(None, "det", None),
        P(),
    )
    ring = mesh.shape["det"]
    shares = mesh.shape["groups"] * mesh.shape["tm"]

    def on_device(tod, gain_knots, intervals, fraction, azimuth, mode_index, mode_bank, mode_mix):
        args = (tod, gain_knots, intervals, fraction, azimuth, mode_index, mode_bank, mode_mix)
        if ring == 4 and mode_index.shape[0] == ring and shares == 8 and mesh.shape["tm"] == 4 and mode_bank.shape[0] == 2 and tod.shape[0] % (16 * shares) == 0:
            return exchanged_blocks(ring, shares, *args)
        return gathered_sums(*args)

    return jax.shard_map(
        on_device, mesh=mesh, in_specs=placed, out_specs=P(("groups", "det"), "tm"), check_vma=False
    )
```

```python
import functools
import jax
import jax.numpy as jnp
from jax import lax
from jax.experimental import pallas as pl
from jax.experimental.pallas import tpu as pltpu
from jax.sharding import PartitionSpec as P

BLOCK = 1024
NBIN = 512
PIECES = ((0, 256), (512, 512), (256, 128), (384, 128))
USED = 448
LATE = 2
GRANT = pltpu.CompilerParams(vmem_limit_bytes=32 * 1024 * 1024)


def gathered_sums(tod, gain_knots, intervals, fraction, azimuth, mode_index, mode_bank, mode_mix):
    precise = lax.Precision.HIGHEST
    det_rows, samples = tod.shape
    knot_row = lax.broadcasted_iota(jnp.int32, (gain_knots.shape[1], samples), 0)
    spread = jnp.where(knot_row == intervals[None, :], 1.0 - fraction[None, :], 0.0)
    spread = spread + jnp.where(knot_row == intervals[None, :] + 1, fraction[None, :], 0.0)
    calibrated = tod * jnp.dot(gain_knots, spread, precision=precise)
    nblocks = samples // BLOCK
    blocks = calibrated.reshape(det_rows, nblocks, BLOCK)
    selected = jnp.take(mode_bank, mode_index, axis=0)
    mixing = jnp.take(mode_mix, mode_index, axis=0)
    partial_amps = jnp.einsum("kdm,dkt->kmt", selected, blocks, precision=precise)
    share = lax.psum_scatter(partial_amps, "det", scatter_dimension=2, tiled=True)
    coef_share = share + jnp.einsum("kmn,knt->kmt", mixing, share, precision=precise)
    coef = lax.all_gather(coef_share, "det", axis=2, tiled=True)
    removed = jnp.einsum("kdm,kmt->dkt", selected, coef, precision=precise)
    cleaned = (blocks - removed).reshape(det_rows, samples)
    onehot = (lax.broadcasted_iota(jnp.int32, (NBIN, samples), 0) == azimuth[None, :]).astype(
        tod.dtype
    )
    fit_part = lax.dot_general(cleaned, onehot, (((1,), (1,)), ((), ())), precision=precise)
    count_part = jnp.sum(onehot, axis=1)
    fit, counts = lax.psum((fit_part, count_part), "tm")
    template = fit / jnp.maximum(counts, 1.0)[None, :]
    return cleaned - jnp.dot(template, onehot, precision=precise)


def halves(x):
    high = x.astype(jnp.bfloat16)
    return high, (x - high.astype(jnp.float32)).astype(jnp.bfloat16)


def dot(a, b, contract=((1,), (0,))):
    return lax.dot_general(a, b, (contract, ((), ())), preferred_element_type=jnp.float32)


def dot3(a, b):
    return dot(a[0], b[0]) + (dot(a[0], b[1]) + dot(a[1], b[0]))


def calibrate_kernel(count, me_ref, gain_ref, *refs):
    gain_high, gain_low = halves(gain_ref[...])
    gains = jnp.concatenate([gain_high, gain_high, gain_low, gain_low], axis=0)
    knots = gain_ref.shape[0]
    for n in range(count):
        tod_ref, where_ref, share_ref = refs[3 * n : 3 * n + 3]
        knot_row = lax.broadcasted_iota(jnp.int32, (knots, tod_ref.shape[1]), 0)
        where, share = where_ref[...], share_ref[...]
        spread = jnp.where(knot_row == where, 1.0 - share, 0.0)
        spread = spread + jnp.where(knot_row == where + 1, share, 0.0)
        high, low = halves(spread)
        spreads = jnp.concatenate([high, low, high, low], axis=0)
        refs[3 * count + n][...] = tod_ref[...] * dot(gains, spreads, ((0,), (0,)))


def calibrate(me, tod, gains, where, share, pieces, grant, place):
    rows = tod.shape[0]
    specs, operands = [], []
    for shift, start, width in pieces:
        per_block, offset = BLOCK // width, start // width

        def at(i, me_ref, shift=shift, per_block=per_block, offset=offset):
            return 0, jnp.bitwise_xor(me_ref[0], shift) * per_block + offset

        specs += [pl.BlockSpec((rows, width), at)] + [pl.BlockSpec((1, width), at)] * 2
        operands += [tod, where, share]
    return pl.pallas_call(
        functools.partial(calibrate_kernel, len(pieces)),
        compiler_params=grant,
        out_shape=[place((rows, width), jnp.float32) for _, _, width in pieces],
        grid_spec=pltpu.PrefetchScalarGridSpec(
            num_scalar_prefetch=1,
            grid=(1,),
            in_specs=[pl.BlockSpec(gains.shape, lambda i, me_ref: (0, 0))] + specs,
            out_specs=[pl.BlockSpec((rows, width), lambda i, me_ref: (0, 0)) for _, _, width in pieces],
        ),
        cost_estimate=pl.CostEstimate(
            flops=2 * rows * 256 * sum(w for _, _, w in pieces),
            bytes_accessed=8 * rows * sum(w for _, _, w in pieces),
            transcendentals=0,
        ),
    )(me, gains, *operands)


def modes_kernel(ring, shares, at_ref, bank_ref, mix_ref, first_high, first_low, second_high, second_low, modes):
    rows = bank_ref.shape[2]
    part = at_ref[2]
    other = pl.program_id(0)
    z_slot = (other // 2) + 2 * lax.rem(other, 2)
    for share in range(shares):
        flip = jnp.bitwise_xor(part, share)
        slot = z_slot + ring * (lax.rem(flip // 2, 2) + 2 * (flip // 4) + 4 * lax.rem(flip, 2))
        modes[pl.ds(share * rows, rows), :] = bank_ref[slot, 0]
    u = modes[...]
    mixed = u + dot3(halves(u), halves(mix_ref[0]))
    first_high[...], first_low[...] = halves(u.T)
    second_high[...], second_low[...] = halves(mixed)


def prepare_modes(ring, shares, at, banks, mode_mix):
    _, _, rows, m = banks.shape
    det_rows = rows * shares
    first = pl.BlockSpec((m, det_rows), lambda s, at_ref: (0, s))
    second = pl.BlockSpec((det_rows, m), lambda s, at_ref: (s, 0))
    total = ring * det_rows
    return pl.pallas_call(
        functools.partial(modes_kernel, ring, shares),
        compiler_params=GRANT,
        out_shape=[jax.ShapeDtypeStruct((m, total), jnp.bfloat16)] * 2
        + [jax.ShapeDtypeStruct((total, m), jnp.bfloat16)] * 2,
        grid_spec=pltpu.PrefetchScalarGridSpec(
            num_scalar_prefetch=1,
            grid=(ring,),
            in_specs=[
                pl.BlockSpec((banks.shape[0], 1, rows, m), lambda s, at_ref: (0, at_ref[1], 0, 0)),
                pl.BlockSpec((1, m, m), lambda s, at_ref: (at_ref[1], 0, 0)),
            ],
            out_specs=[first, first, second, second],
            scratch_shapes=[pltpu.VMEM((det_rows, m), jnp.float32)],
        ),
        cost_estimate=pl.CostEstimate(
            flops=6 * total * m * m, bytes_accessed=12 * total * m, transcendentals=0
        ),
    )(at, banks, mode_mix)


def filter_kernel(ring, first_high, first_low, second_high, second_low, *refs):
    rows = refs[0].shape[0]
    data = halves(jnp.concatenate([refs[s][...] for s in range(ring)], axis=0))
    amps = dot3((first_high[...], first_low[...]), data)
    amps = halves(amps)
    for s in range(ring):
        block = pl.ds(s * rows, rows)
        refs[ring + s][...] = dot3((second_high[block, :], second_low[block, :]), amps)


def common_mode(ring, modes, arrived):
    rows, width = arrived[0].shape
    m, total = modes[0].shape
    tile = min(width, 256)
    whole = [pl.BlockSpec((m, total), lambda i: (0, 0))] * 2 + [pl.BlockSpec((total, m), lambda i: (0, 0))] * 2
    column = pl.BlockSpec((rows, tile), lambda i: (0, i))
    return pl.pallas_call(
        functools.partial(filter_kernel, ring),
        compiler_params=GRANT,
        out_shape=[jax.ShapeDtypeStruct((rows, width), jnp.float32)] * ring,
        grid=(width // tile,),
        in_specs=whole + [column] * ring,
        out_specs=[column] * ring,
        cost_estimate=pl.CostEstimate(
            flops=12 * total * m * width, bytes_accessed=8 * total * width, transcendentals=0
        ),
    )(*modes, *arrived)


def share_kernel(part_ref, bank_ref, out_ref):
    out_ref[0] = bank_ref[...]


def own_share(part, mode_bank, shares):
    count, rows, m = mode_bank.shape
    return pl.pallas_call(
        share_kernel,
        out_shape=pltpu.VMEM((1, count, rows // shares, m), jnp.float32),
        grid_spec=pltpu.PrefetchScalarGridSpec(
            num_scalar_prefetch=1,
            grid=(1,),
            in_specs=[pl.BlockSpec((count, rows // shares, m), lambda i, part_ref: (0, part_ref[0], 0))],
            out_specs=pl.BlockSpec((1, count, rows // shares, m), lambda i, part_ref: (0, 0, 0, 0)),
        ),
    )(part, mode_bank)


def last_kernel(ring, start, at_ref, *refs):
    data, back = refs[:ring], refs[ring : 2 * ring - 1]
    out_ref, held, done = refs[-3:]
    copies = []
    for s in range(ring):
        held[s] = data[s][...] - back[s - 1][...] if s else data[s][...]
        column = pl.ds(block_start(at_ref[0], s, start), held.shape[2])
        copies.append(pltpu.make_async_copy(held.at[s], out_ref.at[:, column], done.at[s]))
        copies[s].start()
    for copy in copies:
        copy.wait()


def last_piece(ring, at, start, data, back, old):
    rows, width = data[0].shape
    return pl.pallas_call(
        functools.partial(last_kernel, ring, start),
        out_shape=jax.ShapeDtypeStruct(old.shape, jnp.float32),
        in_specs=[pl.BlockSpec(memory_space=pltpu.SMEM)]
        + [pl.BlockSpec(memory_space=pltpu.VMEM)] * (2 * ring - 1)
        + [pl.BlockSpec(memory_space=pl.ANY)],
        out_specs=pl.BlockSpec(memory_space=pl.ANY),
        scratch_shapes=[pltpu.VMEM((ring, rows, width), jnp.float32), pltpu.SemaphoreType.DMA((ring,))],
        input_output_aliases={2 * ring: 0},
        compiler_params=GRANT,
        cost_estimate=pl.CostEstimate(
            flops=ring * rows * width, bytes_accessed=12 * ring * rows * width, transcendentals=0
        ),
    )(at, *data, *back, old)


def onehot_of(azimuth, bins):
    row = lax.broadcasted_iota(jnp.int32, (bins, azimuth.shape[1]), 0)
    return (row == azimuth).astype(jnp.float32).astype(jnp.bfloat16)


def block_start(me, shift, start):
    return pl.multiple_of(jnp.bitwise_xor(me, shift) * BLOCK + start, 128)


def bin_kernel(pieces, at_ref, index_ref, azimuth_ref, *refs):
    data, (keep_ref, send_ref, sums) = refs[: len(pieces)], refs[len(pieces) :]
    me, tm = at_ref[0], at_ref[4]
    rows = keep_ref.shape[0]
    sums[...] = jnp.zeros_like(sums)
    for (shift, start, width), ref in zip(pieces, data):
        both = jnp.concatenate(halves(ref[...]), axis=0)
        onehot = onehot_of(azimuth_ref[:, pl.ds(block_start(me, shift, start), width)], sums.shape[2])
        part = dot(both, onehot, ((1,), (1,)))
        sums[index_ref[jnp.bitwise_xor(me, shift)]] += part[:rows] + part[rows:]
    share = sums.shape[2] // 4
    for x in range(2):
        for bank in range(2):
            column = slice((2 * x + bank) * share, (2 * x + bank + 1) * share)
            for flip, ref in ((0, keep_ref), (1, send_ref)):
                first = pl.multiple_of(jnp.bitwise_xor(tm, 2 * x + flip) * share, share)
                ref[:, column] = sums[bank, :, pl.ds(first, share)]


def bin_data(at, mode_index, azimuth, pieces, data):
    rows = data[0].shape[0]
    work = sum(width for _, _, width in pieces)
    return pl.pallas_call(
        functools.partial(bin_kernel, pieces),
        compiler_params=GRANT,
        out_shape=[jax.ShapeDtypeStruct((rows, NBIN), jnp.float32)] * 2,
        in_specs=[pl.BlockSpec(memory_space=pltpu.SMEM)] * 2 + [pl.BlockSpec(memory_space=pltpu.VMEM)] * (1 + len(data)),
        out_specs=[pl.BlockSpec(memory_space=pltpu.VMEM)] * 2,
        scratch_shapes=[pltpu.VMEM((2, rows, NBIN), jnp.float32)],
        cost_estimate=pl.CostEstimate(
            flops=4 * rows * work * NBIN, bytes_accessed=4 * rows * work, transcendentals=0
        ),
    )(at, mode_index, azimuth, *data)


def pool_kernel(ring, shares, at_ref, bank_ref, own_ref, mix_ref, sums_ref, mine_ref, cross_ref, near_ref, total):
    step = pl.program_id(0)
    slots, _, rows, m = bank_ref.shape
    sums = halves(sums_ref[...])
    amps = [halves(own_ref[0].T)[n] for n in range(2)]
    amps = dot3(amps, sums)
    coef = halves(amps + dot3(halves(mix_ref[0]), halves(amps)))
    removed = dot3(halves(bank_ref[:, 0].reshape(slots * rows, m)), coef)

    @pl.when(step == 0)
    def _():
        total[...] = removed
        mine_ref[...] = sums_ref[...]

    @pl.when(step == 1)
    def _():
        total[...] += removed
        mine_ref[...] += sums_ref[...]
        part = at_ref[2]
        for p in range(shares):
            flip = jnp.bitwise_xor(part, p)
            slot = ring * (lax.rem(flip // 2, 2) + 2 * (flip // 4) + 4 * lax.rem(flip, 2))
            block = slice(p * rows, (p + 1) * rows)

            def rows_of(z):
                return total[pl.ds(pl.multiple_of((slot + z) * rows, rows), rows), :]

            mine_ref[block, :] -= rows_of(0)
            cross_ref[block, :] = rows_of(1)
            near_ref[block, :] = rows_of(2)
            near_ref[p * rows + shares * rows : (p + 1) * rows + shares * rows, :] = rows_of(3)


def pool(ring, shares, at, banks, mode_bank, mode_mix, sums):
    slots, _, rows, m = banks.shape
    det_rows, share = rows * shares, sums.shape[1] // 2
    shapes = [(det_rows, share), (det_rows, share), (2 * det_rows, share)]
    return pl.pallas_call(
        functools.partial(pool_kernel, ring, shares),
        compiler_params=GRANT,
        out_shape=[jax.ShapeDtypeStruct(shape, jnp.float32) for shape in shapes],
        grid_spec=pltpu.PrefetchScalarGridSpec(
            num_scalar_prefetch=1,
            grid=(2,),
            in_specs=[
                pl.BlockSpec((slots, 1, rows, m), lambda b, at_ref: (0, b, 0, 0)),
                pl.BlockSpec((1, det_rows, m), lambda b, at_ref: (b, 0, 0)),
                pl.BlockSpec((1, m, m), lambda b, at_ref: (b, 0, 0)),
                pl.BlockSpec((det_rows, share), lambda b, at_ref: (0, b)),
            ],
            out_specs=[pl.BlockSpec(shape, lambda b, at_ref: (0, 0)) for shape in shapes],
            scratch_shapes=[pltpu.VMEM((slots * rows, share), jnp.float32)],
        ),
        cost_estimate=pl.CostEstimate(
            flops=30 * slots * rows * m * share, bytes_accessed=8 * slots * rows * m, transcendentals=0
        ),
    )(at, banks, mode_bank, mode_mix, sums)


def stack_kernel(at_ref, here_ref, there_ref, counts_ref, both_ref):
    tm = at_ref[4]
    rows, width = here_ref.shape
    share = width // 2
    for flip, ref in ((0, here_ref), (1, there_ref)):
        for x in range(2):
            first = pl.multiple_of(jnp.bitwise_xor(tm, 2 * x + flip) * share, share)
            counts = jnp.maximum(counts_ref[:1, pl.ds(first, share)], 1.0)
            high, low = halves(ref[:, x * share : (x + 1) * share] / counts)
            both_ref[:rows, pl.ds(first, share)] = high
            both_ref[rows:, pl.ds(first, share)] = low


def stack_template(at, here, there, counts):
    return pl.pallas_call(
        stack_kernel,
        compiler_params=GRANT,
        out_shape=jax.ShapeDtypeStruct((2 * here.shape[0], NBIN), jnp.bfloat16),
        in_specs=[pl.BlockSpec(memory_space=pltpu.SMEM)] + [pl.BlockSpec(memory_space=pltpu.VMEM)] * 3,
        out_specs=pl.BlockSpec(memory_space=pltpu.VMEM),
    )(at, here, there, counts)


def finish_kernel(ring, at_ref, *refs):
    data, back = refs[:ring], refs[ring : 2 * ring]
    both_ref, azimuth_ref = refs[2 * ring : 2 * ring + 2]
    out_ref = refs[-1]
    rows = out_ref.shape[0]
    levels = dot(both_ref[...], onehot_of(azimuth_ref[...], both_ref.shape[1]))
    levels = levels[:rows] + levels[rows:]
    for s in range(ring):

        @pl.when(pl.program_id(0) == s)
        def _():
            out_ref[...] = data[s][...] - back[s][...] - levels


def finish_piece(ring, at, start, data, back, template, azimuth, old):
    rows, width = data[0].shape
    samples = azimuth.shape[1]
    per_block, offset = BLOCK // width, start // width

    def where(s, at_ref):
        return 0, jnp.bitwise_xor(at_ref[0], s) * per_block + offset

    operands = [*data, *back, template, azimuth]
    specs = [pl.BlockSpec((rows, width), lambda s, at_ref: (0, 0))] * (2 * ring)
    specs += [pl.BlockSpec(template.shape, lambda s, at_ref: (0, 0)), pl.BlockSpec((1, width), where)]
    if old is not None:
        specs += [pl.BlockSpec(memory_space=pl.ANY)]
        operands += [old]
    return pl.pallas_call(
        functools.partial(finish_kernel, ring),
        compiler_params=GRANT,
        out_shape=jax.ShapeDtypeStruct((rows, samples), jnp.float32),
        grid_spec=pltpu.PrefetchScalarGridSpec(
            num_scalar_prefetch=1,
            grid=(ring,),
            in_specs=specs,
            out_specs=pl.BlockSpec((rows, width), where),
        ),
        input_output_aliases={len(operands): 0} if old is not None else {},
        cost_estimate=pl.CostEstimate(
            flops=4 * ring * rows * width * NBIN, bytes_accessed=12 * ring * rows * width, transcendentals=0
        ),
    )(at, *operands)


def level_kernel(ring, start, at_ref, both_ref, azimuth_ref, back_ref, *refs):
    data, outs = refs[:ring], refs[ring:]
    rows, width = outs[0].shape
    for s in range(ring):
        azimuth = azimuth_ref[:, pl.ds(block_start(at_ref[0], s, start), width)]
        levels = dot(both_ref[...], onehot_of(azimuth, both_ref.shape[1]))
        value = data[s][...] - (levels[:rows] + levels[rows:])
        outs[s][...] = value - back_ref[...] if s == 0 else value


def level_piece(ring, at, start, data, back, template, azimuth):
    rows, width = data[0].shape
    return pl.pallas_call(
        functools.partial(level_kernel, ring, start),
        compiler_params=GRANT,
        out_shape=[jax.ShapeDtypeStruct((rows, width), jnp.float32)] * ring,
        in_specs=[pl.BlockSpec(memory_space=pltpu.SMEM)] + [pl.BlockSpec(memory_space=pltpu.VMEM)] * (3 + ring),
        out_specs=[pl.BlockSpec(memory_space=pltpu.VMEM)] * ring,
        cost_estimate=pl.CostEstimate(
            flops=4 * ring * rows * width * NBIN, bytes_accessed=8 * ring * rows * width, transcendentals=0
        ),
    )(at, template, azimuth, back, *data)


def exchanged_blocks(ring, shares, tod, gain_knots, intervals, fraction, azimuth, mode_index, mode_bank, mode_mix):
    det_rows, samples = tod.shape
    me = lax.axis_index("det")
    tm = lax.axis_index("tm")
    part_of = lax.axis_index("groups") * lax.axis_size("tm") + tm
    which = lax.dynamic_index_in_dim(mode_index, me, 0, False)
    me_only = jnp.full((1,), me, jnp.int32)
    at = jnp.stack([me, which, part_of, lax.rem(tm, 2), tm])

    def swap(array, axis, bit):
        return lax.ppermute(array, axis, [(i, i ^ bit) for i in range(lax.axis_size(axis))])

    gains = gain_knots.T
    where, share = intervals[None, :], fraction[None, :]
    share_bins, used = NBIN // lax.axis_size("tm"), USED // lax.axis_size("tm")
    azimuth = azimuth[None, :]
    azimuth = azimuth + (share_bins - used) * sum((azimuth >= n * used).astype(jnp.int32) for n in range(1, NBIN // share_bins))
    data, arrived = {}, {}
    order = [[(s, start, width) for s in (1, 2, 3)] for start, width in PIECES]
    order[-1] += [(0, start, width) for start, width in PIECES]
    for part, pieces in enumerate(order):
        grant = GRANT if part else pltpu.CompilerParams()
        place = jax.ShapeDtypeStruct if part else pltpu.VMEM
        blocks = calibrate(me_only, tod, gains, where, share, pieces, grant, place)
        for (s, start, width), block in zip(pieces, blocks):
            data[s, start] = block
            arrived[s, start] = swap(block, "det", s) if s else block

    banks = own_share(jnp.full((1,), part_of, jnp.int32), mode_bank, shares)
    for bit in (2, 1):
        banks = jnp.concatenate([banks, swap(banks, "det", bit)], axis=0)
    by_x = swap(banks, "tm", 2)
    by_y = swap(banks, "groups", 1)
    diagonal = [swap(by_x[:2], "groups", 1), swap(by_y[2:], "tm", 2)]
    banks = jnp.concatenate([banks, by_x, by_y, *diagonal], axis=0)
    banks = jnp.concatenate([banks, swap(banks, "tm", 1)], axis=0)

    pieces = [piece for part in order for piece in part]
    keep, other = bin_data(at, mode_index, azimuth, pieces, [data[s, start] for s, start, _ in pieces])
    sums = keep + swap(other, "tm", 1)
    half = NBIN // 2
    sums = sums[:, :half] + swap(sums[:, half:], "tm", 2)
    mine, cross, near = pool(ring, shares, at, banks, mode_bank, mode_mix, sums)
    near = swap(near, "det", 1)
    cross = swap((cross + near[det_rows:]).T[:used], "det", 2)
    template = mine - near[:det_rows] - jnp.pad(cross, ((0, share_bins - used), (0, 0))).T
    template = jnp.concatenate([template, swap(template, "tm", 2)], axis=1)
    other = swap(template, "tm", 1)

    counts = jnp.sum((lax.broadcasted_iota(jnp.int32, (NBIN, samples), 0) == azimuth).astype(jnp.float32), axis=1)
    counts = jnp.broadcast_to(counts[None, :], (8, NBIN))
    for bit in (1, 2):
        counts = counts + swap(counts, "tm", bit)
    template = stack_template(at, template, other, counts)

    modes = prepare_modes(ring, shares, at, banks, mode_mix)
    out = None
    for part, (start, width) in enumerate(PIECES):
        removed = common_mode(ring, modes, [arrived[s, start] for s in range(ring)])
        back = [swap(removed[s], "det", s) if s else removed[s] for s in range(ring)]
        mine = [data[s, start] for s in range(ring)]
        if part < len(PIECES) - LATE:
            out = finish_piece(ring, at, start, mine, back, template, azimuth, out)
        else:
            mine = level_piece(ring, at, start, mine, back[0], template, azimuth)
            out = last_piece(ring, at, start, mine, back[1:], out)
    return out


def solution(mesh):
    placed = (
        P(("groups", "det"), "tm"),
        P(("groups", "det"), None),
        P(("groups", "tm")),
        P(("groups", "tm")),
        P(("groups", "tm")),
        P(("groups", "tm")),
        P(None, "det", None),
        P(),
    )
    ring = mesh.shape["det"]
    shares = mesh.shape["groups"] * mesh.shape["tm"]

    def on_device(tod, gain_knots, intervals, fraction, azimuth, mode_index, mode_bank, mode_mix):
        args = (tod, gain_knots, intervals, fraction, azimuth, mode_index, mode_bank, mode_mix)
        if ring == 4 and mode_index.shape[0] == ring and shares == 8 and mesh.shape["tm"] == 4 and mode_bank.shape[0] == 2 and tod.shape[0] % (16 * shares) == 0:
            return exchanged_blocks(ring, shares, *args)
        return gathered_sums(*args)

    return jax.shard_map(
        on_device, mesh=mesh, in_specs=placed, out_specs=P(("groups", "det"), "tm"), check_vma=False
    )
```
